128 devices in a mesh: gx: 8 (over y, core), gy: 16 (over x, z).
Axes of the slice: x: 4, y: 4, z: 4, core: 2. Of those that a mesh axis runs over, the one named last changes fastest.
Arguments:
- voxels_fine: bfloat16 [1024, 64, 512], P(('gx', 'gy')), may hold values from -6 to 6
- gain_fine: float32 [64], replicated, may hold values from 0.5 to 2
- gain_middle: float32 [128], replicated, may hold values from 0.5 to 2
- gain_coarse: float32 [256], replicated, may hold values from 0.5 to 2
- kernel_fine: bfloat16 [27, 64, 64], replicated, may hold values from -0.15625 to 0.15625
- kernel_middle: bfloat16 [27, 128, 128], replicated, may hold values from -0.109375 to 0.109375
- kernel_coarse: bfloat16 [27, 256, 256], replicated, may hold values from -0.078125 to 0.078125
- lift_middle: bfloat16 [128, 64], replicated, may hold values from -0.75 to 0.75
- lift_coarse: bfloat16 [256, 128], replicated, may hold values from -0.5 to 0.5
- links_fine: int32 [1024, 26], P(('gx', 'gy')), may hold values from 0 to 1072, as said below
- links_middle: int32 [256, 26], P(('gx', 'gy')), may hold values from 0 to 524, as said below
- links_coarse: int32 [128, 26], P(('gx', 'gy')), may hold values from 0 to 262, as said below
- sends_fine: int32 [128, 1024], P(('gx', 'gy')), may hold values from -1 to 47, as said below
- sends_middle: int32 [128, 512], P(('gx', 'gy')), may hold values from -1 to 11, as said below
- sends_coarse: int32 [128, 256], P(('gx', 'gy')), may hold values from -1 to 5, as said below
- parents_middle: int32 [256, 8], P(('gx', 'gy')), may hold values from 0 to 136
- parents_coarse: int32 [128, 8], P(('gx', 'gy')), may hold values from 0 to 130
- uplinks_middle: int32 [128, 128], P(('gx', 'gy')), may hold values from -1 to 7, as said below
- uplinks_coarse: int32 [128, 128], P(('gx', 'gy')), may hold values from -1 to 1, as said below
Outputs:
- output_fine: bfloat16 [1024, 64, 512], P(('gx', 'gy'))
- output_middle: bfloat16 [256, 128, 512], P(('gx', 'gy'))
- output_coarse: bfloat16 [128, 256, 512], P(('gx', 'gy'))
The draws below stay inside these ranges and needn't reach their ends.
Inputs may be any that keep to these rules, and one draw needn't show every extreme that they name: `links_fine`: rows 48 and up name received slabs or the zero row of the step. `links_middle`: rows 12 and up name received slabs or the zero row of the step. `links_coarse`: rows 6 and up name received slabs or the zero row of the step. `sends_fine`: -1 marks an empty slot. `sends_middle`: -1 marks an empty slot. `sends_coarse`: -1 marks an empty slot. `uplinks_middle`: -1 marks an empty slot. `uplinks_coarse`: -1 marks an empty slot.
All inputs are finite; a program needn't handle non-finite values.
Results may differ from the reference program's by a relative error of at most 0.015.
Values may be sent and summed in bfloat16 or wider, within the bound.
A program may use at most 192 MiB of HBM per device.

```python
import math
import jax
import jax.numpy as jnp
from jax import lax

C0 = 64
C1 = 128
C2 = 256
B0_DEV = 8
SLOTS0 = 8
SLOTS1 = 4
SLOTS2 = 2
POOL_SLOTS = 1
B1_DEV = 2
B2_DEV = 1
NB0 = 1024
DEVICES = 128


DIRECTIONS = [(along_x, along_y, along_z) for along_x in (-1, 0, 1) for along_y in (-1, 0, 1) for along_z in (-1, 0, 1) if (along_x, along_y, along_z) != (0, 0, 0)]


def face_index(direction):
    for position in range(3):
        if direction[position] != 0:
            return 2 * position + (0 if direction[position] < 0 else 1)
    return 0


def face_ids():
    return jnp.array([face_index(direction) for direction in DIRECTIONS], jnp.int32)


def link_tables(key, bricks, ways, slot_count, remote_pct, stride, offsets, local_width):
    members = DEVICES
    total_rows = members * bricks
    keys = jax.random.split(key, 8)
    device = (jnp.arange(total_rows, dtype=jnp.int32) // bricks)[:, None]
    rolled = jax.random.randint(keys[0], (total_rows, ways), 0, 100)
    nearby = jax.random.randint(keys[1], (total_rows, ways), 1, 5) * (2 * jax.random.randint(keys[2], (total_rows, ways), 0, 2) - 1)
    distant = jax.random.randint(keys[3], (total_rows, ways), 1, members)
    picker = jax.random.randint(keys[4], (total_rows, ways), 0, 100)
    offset = jnp.where(picker < 60, nearby, distant)
    owner = (device + offset + members) % members
    slot = jax.random.randint(keys[5], (total_rows, ways), 0, slot_count)
    local = jax.random.randint(keys[6], (total_rows, ways), 0, local_width // stride) * stride + offsets[None, :]
    remote = rolled < remote_pct
    empty = rolled >= 90
    table = jnp.where(remote, local_width + owner * slot_count + slot, jnp.where(empty, local_width + members * slot_count, local))
    receiver = jnp.broadcast_to(device, (total_rows, ways)).reshape(-1)
    column = (owner * slot_count + slot).reshape(-1)
    usable = jnp.zeros((members, members * slot_count), jnp.int32).at[receiver, column].max(remote.reshape(-1).astype(jnp.int32))
    usable = usable.reshape(members, members, slot_count).transpose(1, 0, 2).reshape(members, members * slot_count)
    chosen = jax.random.randint(keys[7], (members, members * slot_count), 0, local_width)
    senders = jnp.where(usable > 0, chosen, -1)
    return (table.astype(jnp.int32), senders.astype(jnp.int32))


def fine_tables(key):
    return link_tables(jax.random.fold_in(key, 11), B0_DEV, 26, SLOTS0, 60, 6, face_ids(), 6 * B0_DEV)


def middle_tables(key):
    return link_tables(jax.random.fold_in(key, 12), B1_DEV, 26, SLOTS1, 60, 6, face_ids(), 6 * B1_DEV)


def coarse_tables(key):
    return link_tables(jax.random.fold_in(key, 13), B2_DEV, 26, SLOTS2, 88, 6, face_ids(), 6 * B2_DEV)


def middle_parents(key):
    return link_tables(jax.random.fold_in(key, 21), B1_DEV, 8, POOL_SLOTS, 60, 1, jnp.zeros((8,), jnp.int32), B0_DEV)


def coarse_parents(key):
    return link_tables(jax.random.fold_in(key, 22), B2_DEV, 8, POOL_SLOTS, 60, 1, jnp.zeros((8,), jnp.int32), B1_DEV)


def draw_links_fine(key, part):
    return fine_tables(key)[0]


def draw_sends_fine(key, part):
    return fine_tables(key)[1]


def draw_links_middle(key, part):
    return middle_tables(key)[0]


def draw_sends_middle(key, part):
    return middle_tables(key)[1]


def draw_links_coarse(key, part):
    return coarse_tables(key)[0]


def draw_sends_coarse(key, part):
    return coarse_tables(key)[1]


def draw_parents_middle(key, part):
    return middle_parents(key)[0]


def draw_uplinks_middle(key, part):
    return middle_parents(key)[1]


def draw_parents_coarse(key, part):
    return coarse_parents(key)[0]


def draw_uplinks_coarse(key, part):
    return coarse_parents(key)[1]


def level_of(own_key, extent, cuts, low, top_value):
    factor_of, own = 1.0, jax.random.fold_in(own_key, 6)
    for dim, shards_of in cuts:
        draws = jnp.exp(jax.random.uniform(jax.random.fold_in(own, dim), (shards_of,), jnp.float32, low / len(cuts), top_value / len(cuts)))
        factor_of = factor_of * jnp.repeat(draws, extent[dim] // shards_of).reshape([-1 if axis == dim else 1 for axis in range(len(extent))])
    return factor_of


def bell_draw(own_key, shape, deviation, most, cuts=(), held_as=jnp.bfloat16):
    drawn = deviation * jax.random.normal(own_key, shape, jnp.float32)
    if cuts:
        drawn = drawn * level_of(own_key, shape, cuts, -0.22, 0.18)
    return jnp.clip(drawn, -most, most).astype(held_as)


def setup_inputs(seed: int = 0) -> dict:
    key_of = jax.random.split(jax.random.key(seed), 20)
    voxels_fine = bell_draw(key_of[0], (NB0, C0, 512), 1.0, 6.0, ((0, 128),))
    gain_fine = jnp.clip(jnp.exp(jax.random.uniform(key_of[1], (C0,), jnp.float32, math.log(0.5), math.log(2.0))), 0.5, 2.0)
    gain_middle = jnp.clip(jnp.exp(jax.random.uniform(key_of[2], (C1,), jnp.float32, math.log(0.5), math.log(2.0))), 0.5, 2.0)
    gain_coarse = jnp.clip(jnp.exp(jax.random.uniform(key_of[3], (C2,), jnp.float32, math.log(0.5), math.log(2.0))), 0.5, 2.0)
    kernel_fine = bell_draw(key_of[4], (27, C0, C0), (27 * C0) ** -0.5, 0.15625)
    kernel_middle = bell_draw(key_of[5], (27, C1, C1), (27 * C1) ** -0.5, 0.109375)
    kernel_coarse = bell_draw(key_of[6], (27, C2, C2), (27 * C2) ** -0.5, 0.078125)
    lift_middle = bell_draw(key_of[7], (C1, C0), C0 ** -0.5, 0.75)
    lift_coarse = bell_draw(key_of[8], (C2, C1), C1 ** -0.5, 0.5)
    links_fine = draw_links_fine(jax.random.fold_in(key_of[19], 71), 0)
    links_middle = draw_links_middle(jax.random.fold_in(key_of[19], 71), 0)
    links_coarse = draw_links_coarse(jax.random.fold_in(key_of[19], 71), 0)
    sends_fine = draw_sends_fine(jax.random.fold_in(key_of[19], 71), 0)
    sends_middle = draw_sends_middle(jax.random.fold_in(key_of[19], 71), 0)
    sends_coarse = draw_sends_coarse(jax.random.fold_in(key_of[19], 71), 0)
    parents_middle = draw_parents_middle(jax.random.fold_in(key_of[19], 71), 0)
    parents_coarse = draw_parents_coarse(jax.random.fold_in(key_of[19], 71), 0)
    uplinks_middle = draw_uplinks_middle(jax.random.fold_in(key_of[19], 71), 0)
    uplinks_coarse = draw_uplinks_coarse(jax.random.fold_in(key_of[19], 71), 0)
    return dict(voxels_fine=voxels_fine, gain_fine=gain_fine, gain_middle=gain_middle, gain_coarse=gain_coarse, kernel_fine=kernel_fine, kernel_middle=kernel_middle, kernel_coarse=kernel_coarse, lift_middle=lift_middle, lift_coarse=lift_coarse, links_fine=links_fine, links_middle=links_middle, links_coarse=links_coarse, sends_fine=sends_fine, sends_middle=sends_middle, sends_coarse=sends_coarse, parents_middle=parents_middle, parents_coarse=parents_coarse, uplinks_middle=uplinks_middle, uplinks_coarse=uplinks_coarse)


EPSILON = 1e-06
DIRECTIONS = [(along_x, along_y, along_z) for along_x in (-1, 0, 1) for along_y in (-1, 0, 1) for along_z in (-1, 0, 1) if (along_x, along_y, along_z) != (0, 0, 0)]
OFFSETS = [along_x * 100 + along_y * 10 + along_z for along_x in range(3) for along_y in range(3) for along_z in range(3)]

def leading_axis(direction):
    for position in range(3):
        if direction[position] != 0:
            return position
    return 0

def activate(hidden, scales):
    values = hidden.astype(jnp.float32)
    mean_sq = lax.optimization_barrier(jnp.mean(values * values, axis=1, keepdims=True))
    scaled = values * lax.rsqrt(mean_sq + EPSILON) * scales[None, :, None]
    return jax.nn.silu(scaled).astype(jnp.bfloat16)

def brick_faces(active):
    bricks, channels = (active.shape[0], active.shape[1])
    volume = active.reshape(bricks, channels, 8, 8, 8)
    layers = [volume[:, :, 7], volume[:, :, 0], volume[:, :, :, 7], volume[:, :, :, 0], volume[:, :, :, :, 7], volume[:, :, :, :, 0]]
    return jnp.stack(layers, axis=1).reshape(bricks * 6, channels * 64)

def assemble(active, slabs):
    bricks, channels = (active.shape[0], active.shape[1])
    padded = jnp.zeros((bricks, channels, 10, 10, 10), active.dtype)
    padded = padded.at[:, :, 1:9, 1:9, 1:9].set(active.reshape(bricks, channels, 8, 8, 8))
    for placing, direction in enumerate(DIRECTIONS):
        slab_cut = slabs[:, placing].reshape(bricks, channels, 8, 8)
        leading = leading_axis(direction)
        others = [position for position in range(3) if position != leading]
        chosen = tuple((slice(None) if direction[position] == 0 else 7 if direction[position] < 0 else 0 for position in others))
        target = tuple((slice(1, 9) if direction[position] == 0 else 0 if direction[position] < 0 else 9 for position in range(3)))
        padded = padded.at[(slice(None), slice(None)) + target].set(slab_cut[(slice(None), slice(None)) + chosen])
    return padded.reshape(bricks, channels, 1000)

def interior(full):
    bricks, outputs = (full.shape[0], full.shape[1])
    widened = jnp.pad(full, ((0, 0), (0, 0), (0, 22)))
    lattice = widened.reshape(bricks, outputs, 8, 100)[:, :, :, :80].reshape(bricks, outputs, 8, 8, 10)[:, :, :, :, :8]
    return lattice.reshape(bricks, outputs, 512)

def convolve(padded, kernel):
    bricks, channels = (padded.shape[0], padded.shape[1])
    outputs = kernel.shape[1]
    columns = jnp.stack([padded[:, :, offset:offset + 778] for offset in OFFSETS], axis=1).reshape(bricks, 27 * channels, 778)
    flat_kernel = kernel.transpose(1, 0, 2).reshape(outputs, 27 * channels)
    full = jnp.einsum('ok,bkv->bov', flat_kernel.astype(jnp.float32), columns.astype(jnp.float32))
    return interior(full)

def pool_blocks(output):
    bricks, channels = (output.shape[0], output.shape[1])
    values = output.astype(jnp.float32).reshape(bricks, channels, 4, 2, 4, 2, 4, 2)
    return lax.optimization_barrier(jnp.mean(values, axis=(3, 5, 7))).astype(jnp.bfloat16).reshape(bricks, channels * 64)

def place_octants(gathered):
    parents = gathered.shape[0]
    channels = gathered.shape[2] // 64
    volume = gathered.reshape(parents, 2, 2, 2, channels, 4, 4, 4)
    return volume.transpose(0, 4, 1, 5, 2, 6, 3, 7).reshape(parents, channels, 512)

def resolve(link_rows, senders, device, local_width):
    members = senders.shape[0]
    slot_count = senders.shape[1] // members
    is_local = link_rows < local_width
    remote = link_rows - local_width
    is_remote = jnp.logical_and(remote >= 0, remote < members * slot_count)
    bounded = jnp.clip(remote, 0, members * slot_count - 1)
    owner = bounded // slot_count
    picked = senders[owner, device * slot_count + bounded % slot_count]
    global_row = jnp.where(is_local, device * local_width + link_rows, owner * local_width + picked)
    usable = jnp.logical_or(is_local, jnp.logical_and(is_remote, picked >= 0))
    return (jnp.where(usable, global_row, 0).astype(jnp.int32), usable)

def halo_level(hidden, scales, kernel, links, senders):
    members = senders.shape[0]
    bricks = hidden.shape[0] // members
    channels = hidden.shape[1]
    active = lax.map(lambda portion: activate(portion, scales), hidden.reshape(members, bricks, channels, 512)).reshape(hidden.shape)
    faces = brick_faces(active)

    def per_device(device):
        link_rows = lax.dynamic_slice_in_dim(links, device * bricks, bricks, 0)
        global_row, usable = resolve(link_rows, senders, device, 6 * bricks)
        slabs = jnp.where(usable.reshape(-1, 1), jnp.take(faces, global_row.reshape(-1), axis=0), jnp.zeros((), faces.dtype))
        mine = lax.dynamic_slice_in_dim(hidden, device * bricks, bricks, 0)
        mine_active = lax.dynamic_slice_in_dim(active, device * bricks, bricks, 0)
        padded = assemble(mine_active, slabs.reshape(bricks, 26, channels * 64))
        return (mine.astype(jnp.float32) + convolve(padded, kernel)).astype(jnp.bfloat16)
    return lax.map(per_device, jnp.arange(members, dtype=jnp.int32)).reshape(hidden.shape)

def pool_level(output, lift, links, senders):
    members = senders.shape[0]
    children = output.shape[0] // members
    parents = links.shape[0] // members
    channels = output.shape[1]
    blocks = lax.map(pool_blocks, output.reshape(members, children, channels, 512)).reshape(members * children, channels * 64)

    def per_device(device):
        link_rows = lax.dynamic_slice_in_dim(links, device * parents, parents, 0)
        global_row, usable = resolve(link_rows, senders, device, children)
        gathered = jnp.where(usable.reshape(-1, 1), jnp.take(blocks, global_row.reshape(-1), axis=0), jnp.zeros((), blocks.dtype))
        parent_grid = place_octants(gathered.reshape(parents, 8, channels * 64))
        return jnp.einsum('oc,bcv->bov', lift.astype(jnp.float32), parent_grid.astype(jnp.float32)).astype(jnp.bfloat16)
    return lax.map(per_device, jnp.arange(members, dtype=jnp.int32)).reshape(members * parents, lift.shape[0], 512)

def reference(voxels_fine, gain_fine, gain_middle, gain_coarse, kernel_fine, kernel_middle, kernel_coarse, lift_middle, lift_coarse, links_fine, links_middle, links_coarse, sends_fine, sends_middle, sends_coarse, parents_middle, parents_coarse, uplinks_middle, uplinks_coarse):
    output_fine = halo_level(voxels_fine, gain_fine, kernel_fine, links_fine, sends_fine)
    hidden_middle = pool_level(output_fine, lift_middle, parents_middle, uplinks_middle)
    output_middle = halo_level(hidden_middle, gain_middle, kernel_middle, links_middle, sends_middle)
    hidden_coarse = pool_level(output_middle, lift_coarse, parents_coarse, uplinks_coarse)
    output_coarse = halo_level(hidden_coarse, gain_coarse, kernel_coarse, links_coarse, sends_coarse)
    return (output_fine, output_middle, output_coarse)
```

```python
import functools

import jax
import jax.numpy as jnp
import numpy as np
from jax import lax
from jax.experimental import pallas as pl
from jax.experimental.pallas import tpu as pltpu
from jax.sharding import PartitionSpec as P

EPSILON = 1e-06
MESH = pl.DeviceIdType.MESH
BF16, F32, I32 = jnp.bfloat16, jnp.float32, jnp.int32
RING = 4
CORES = 2
VMEM_LIMIT = 60 * 1024 * 1024
DIRECTIONS = [
    (a, b, c) for a in (-1, 0, 1) for b in (-1, 0, 1) for c in (-1, 0, 1) if (a, b, c) != (0, 0, 0)
]


def face_sources():
    ids = np.arange(512).reshape(8, 8, 8)
    layers = [ids[7], ids[0], ids[:, 7], ids[:, 0], ids[:, :, 7], ids[:, :, 0]]
    return np.stack(layers).reshape(1, 384).astype(np.int32)


def halo_cells():
    return [
        (x, y, z)
        for x in range(10)
        for y in range(10)
        for z in range(10)
        if not all(1 <= v <= 8 for v in (x, y, z))
    ]


def halo_sources():
    out = np.full((1, 512), -1, np.int32)
    for n, cell in enumerate(halo_cells()):
        t = tuple(-1 if v == 0 else 1 if v == 9 else 0 for v in cell)
        lead = next(p for p in range(3) if t[p] != 0)
        u, v = [7 if t[p] < 0 else 0 if t[p] > 0 else cell[p] - 1 for p in range(3) if p != lead]
        out[0, n] = DIRECTIONS.index(t) * 64 + u * 8 + v
    return out


def padded_sources():
    out = np.full((1, 1280), -1, np.int32)
    halo = {cell: n for n, cell in enumerate(halo_cells())}
    for x in range(10):
        for y in range(10):
            for z in range(10):
                if (x, y, z) in halo:
                    source = 512 + halo[x, y, z]
                else:
                    source = (x - 1) * 64 + (y - 1) * 8 + z - 1
                out[0, x * 128 + y * 10 + z] = source
    return out


def shift_sources():
    out = np.zeros((9, 2, 8, 8), np.int32)
    for d in range(9):
        for q in range(2):
            for y in range(8):
                for z in range(8):
                    out[d, q, y, z] = q * 128 + (y + d // 3) * 10 + z + d % 3
    return out.reshape(1, 1152)


def octant_sources():
    out = np.zeros((8, 8, 8), np.int32)
    for x in range(8):
        for y in range(8):
            for z in range(8):
                octant = 4 * (x // 4) + 2 * (y // 4) + z // 4
                out[x, y, z] = octant * 64 + (x % 4) * 16 + (y % 4) * 4 + z % 4
    return out.reshape(1, 512)


def selection(depth, sources):
    rows = lax.broadcasted_iota(I32, (depth, sources.shape[1]), 0)
    return jnp.where(rows == sources, 1.0, 0.0).astype(BF16)


def mm(a, b):
    return jnp.dot(a, b, preferred_element_type=F32)


def activate(values, gain):
    mean_sq = jnp.mean(values * values, axis=0, keepdims=True)
    scaled = values * lax.rsqrt(mean_sq + EPSILON) * gain
    return (scaled / (1.0 + jnp.exp(-scaled))).astype(BF16)


def write_faces(bricks, channels, active_ref, sources_ref, table_ref):
    faces = mm(active_ref[...], selection(512, sources_ref[...])).astype(BF16)
    for b in range(bricks):
        for pair in range(3):
            table_ref[3 * b + pair] = faces[
                b * channels : (b + 1) * channels, pair * 128 : (pair + 1) * 128
            ]


def enter_fine(bricks, channels, hidden_ref, gain_ref, sources_ref, active_ref, table_ref):
    for b in range(bricks):
        rows = slice(b * channels, (b + 1) * channels)
        active_ref[rows] = activate(hidden_ref[rows].astype(F32), gain_ref[...])
    write_faces(bricks, channels, active_ref, sources_ref, table_ref)


def enter_coarser(
    bricks, below, channels, parts_ref, lift_ref, gain_ref, sources_ref, hidden_ref, active_ref, table_ref
):
    for b in range(bricks):
        own = slice(b * below, (b + 1) * below)
        rows = slice(b * channels, (b + 1) * channels)
        grid = sum(parts_ref[x, own].astype(F32) for x in range(RING)).astype(BF16)
        hidden = mm(lift_ref[...], grid).astype(BF16)
        hidden_ref[rows] = hidden
        active_ref[rows] = activate(hidden.astype(F32), gain_ref[...])
    write_faces(bricks, channels, active_ref, sources_ref, table_ref)


def pack(
    bricks, channels, tiles, ways, index_ref, table_hbm, sources_ref, out_ref, table_ref, gathered_ref, choose_ref, sem
):
    dest = pl.program_id(0)

    @pl.when(dest == 0)
    def _():
        copy = pltpu.make_async_copy(table_hbm, table_ref.at[pl.ds(0, tiles)], sem)
        copy.start()
        table_ref[tiles] = jnp.zeros((channels, 128), BF16)
        choose_ref[...] = selection(ways * 64, sources_ref[...])
        copy.wait()

    lanes = lax.broadcasted_iota(I32, (channels, 128), 1)
    low = lanes < 64

    def brick(b, carry):
        rows = pl.ds(pl.multiple_of(b * channels, channels), channels)
        for way in range(0, ways, 2):
            base = (dest * bricks + b) * ways + way
            first, second = index_ref[base], index_ref[base + 1]
            one = table_ref[first // 2]
            two = table_ref[second // 2]
            one_turned = jnp.concatenate([one[:, 64:], one[:, :64]], axis=1)
            two_turned = jnp.concatenate([two[:, 64:], two[:, :64]], axis=1)
            one = jnp.where(first % 2 == 0, one, one_turned)
            two = jnp.where(second % 2 == 0, two_turned, two)
            gathered_ref[rows, way * 64 : way * 64 + 128] = jnp.where(low, one, two)
        return carry

    lax.fori_loop(0, bricks, brick, 0)
    out_ref[0] = mm(gathered_ref[...], choose_ref[...]).astype(BF16)


def leave(
    bricks,
    channels,
    pooled,
    active_ref,
    parts_ref,
    hidden_ref,
    kernel_ref,
    place_ref,
    shift_ref,
    out_ref,
    *rest,
):
    if pooled:
        table_ref, rest = rest[0], rest[1:]
    source_ref, padded_ref, shifts_ref, weight_ref, moved_ref = rest
    source_ref[:, 0:512] = active_ref[...]
    source_ref[:, 512:1024] = sum(parts_ref[x].astype(F32) for x in range(RING)).astype(BF16)
    padded_ref[...] = mm(source_ref[...], selection(1024, place_ref[...])).astype(BF16)
    shifts_ref[...] = selection(256, shift_ref[...])
    for dx in range(3):
        for d in range(9):
            weight_ref[
                dx * channels : (dx + 1) * channels, d * channels : (d + 1) * channels
            ] = kernel_ref[dx * 9 + d]

    def brick(b, carry):
        start = b * channels if isinstance(b, int) else pl.multiple_of(b * channels, channels)
        rows = pl.ds(start, channels)
        planes = jnp.concatenate(
            [padded_ref[rows, pair * 256 : (pair + 1) * 256] for pair in range(5)], axis=0
        )
        moved = mm(planes, shifts_ref[...]).astype(BF16)
        for pair in range(5):
            for d in range(9):
                moved_ref[d * channels : (d + 1) * channels, pair * 128 : (pair + 1) * 128] = moved[
                    pair * channels : (pair + 1) * channels, d * 128 : (d + 1) * 128
                ]
        total = hidden_ref[rows].astype(F32)
        for dx in range(3):
            part = mm(weight_ref[dx * channels : (dx + 1) * channels], moved_ref[...])
            total = total + part[:, dx * 64 : dx * 64 + 512]
        out_ref[rows] = total.astype(BF16)
        return carry

    if bricks > 1:
        lax.fori_loop(0, bricks, brick, 0)
    else:
        brick(0, 0)
    if pooled:
        voxel = lax.broadcasted_iota(I32, (512, 64), 0)
        block = (
            lax.shift_left(lax.shift_right_logical(voxel, 7), 4)
            + lax.shift_left(lax.shift_right_logical(voxel, 4) & 3, 2)
            + (lax.shift_right_logical(voxel, 1) & 3)
        )
        column = lax.broadcasted_iota(I32, (512, 64), 1)
        average = jnp.where(block == column, 0.125, 0.0).astype(BF16)
        blocks = mm(out_ref[...], average).astype(BF16)
        for b in range(bricks):
            table_ref[b // 2, :, (b % 2) * 64 : (b % 2) * 64 + 64] = blocks[
                b * channels : (b + 1) * channels
            ]


def shape(*dims, dtype=BF16):
    return jax.ShapeDtypeStruct(dims, dtype)


def whole(count):
    return [pl.BlockSpec(memory_space=pltpu.VMEM)] * count


PARAMS = pltpu.CompilerParams(vmem_limit_bytes=VMEM_LIMIT)


def place_self():
    across, along = lax.axis_index("gx"), lax.axis_index("gy")
    return across // CORES, across % CORES, along // RING, along % RING


def gather_kernel(rows, channels, own_ref, all_ref, stage_ref, send_sems, recv_sems, local_sems):
    y, core, x, z = place_self()
    half, quarter = channels // 2, channels // 4

    def peer(dy, dz, other=False):
        new_core = 1 - core if other else core
        return (((y + dy) % RING) * CORES + new_core, x * RING + (z + dz) % RING)

    def slot(dy, dz, other=False):
        new_core = 1 - core if other else core
        return (((y + dy) % RING) * CORES + new_core) * RING + (z + dz) % RING

    barrier = pltpu.get_barrier_semaphore()
    neighbours = [peer(1, 0), peer(3, 0), peer(0, 1), peer(0, 3), peer(0, 0, True)]
    for device in neighbours:
        pl.semaphore_signal(barrier, inc=1, device_id=device, device_id_type=MESH)

    come = pltpu.make_async_copy(own_ref, stage_ref, local_sems.at[0])
    come.start()
    pl.semaphore_wait(barrier, len(neighbours))

    started = []
    counter = [0]

    def send(dy, dz, start, size, device):
        n = counter[0]
        counter[0] += 1
        part = pl.ds(start, size)
        source = own_ref.at[:, part] if (dy, dz) == (0, 0) else all_ref.at[slot(dy, dz), :, part]
        copy = pltpu.make_async_remote_copy(
            src_ref=source,
            dst_ref=all_ref.at[slot(dy, dz), :, part],
            send_sem=send_sems.at[n],
            recv_sem=recv_sems.at[n],
            device_id=device,
            device_id_type=MESH,
        )
        copy.start()
        started.append(copy)
        return n

    def arrived(n, dy, dz, start, size, other=False):
        view = all_ref.at[slot(dy, dz, other), :, pl.ds(start, size)]
        pltpu.make_async_remote_copy(
            src_ref=view,
            dst_ref=view,
            send_sem=send_sems.at[n],
            recv_sem=recv_sems.at[n],
            device_id=neighbours[0],
            device_id_type=MESH,
        ).wait_recv()

    def sibling(dy, dz, start, size):
        n = send(dy, dz, start, size, neighbours[4])
        siblings.append((n, dy, dz, start, size))

    siblings = []
    UP, DOWN = 1, 3

    def off(axis, k):
        return (k % RING, 0) if axis == "y" else (0, k % RING)

    def both(axis, dy, dz, start, size):
        events = []
        for step in (UP, DOWN):
            sy, sz = off(axis, step)
            n = send(dy, dz, start, size, peer(sy, sz))
            events.append((n, axis, step, (dy - sy) % RING, (dz - sz) % RING, start, size))
        return events

    def relay(event):
        n, axis, step, dy, dz, start, size = event
        piece = size // 2
        begin = start if step == UP else start + piece
        sy, sz = off(axis, step)
        m = send(dy, dz, begin, piece, peer(sy, sz))
        return (m, axis, step, (dy - sy) % RING, (dz - sz) % RING, begin, piece)

    def wait(event):
        n, axis, step, dy, dz, start, size = event
        arrived(n, dy, dz, start, size)

    parts = [("z", "y", 0), ("y", "z", half)]
    first, second = [], []
    for axis, other_axis, start in parts:
        first.append(both(axis, 0, 0, start, half))
    for axis, other_axis, start in parts:
        second += both(other_axis, 0, 0, start, half)
    sibling(0, 0, 0, channels)
    come.wait()
    go = pltpu.make_async_copy(stage_ref, all_ref.at[slot(0, 0)], local_sems.at[1])
    go.start()

    relays = []
    for (axis, other_axis, start), events in zip(parts, first):
        passed = []
        for event in events:
            wait(event)
            passed.append(relay(event))
            _, _, _, dy, dz, _, _ = event
            second += both(other_axis, dy, dz, start, half)
            sibling(dy, dz, start, half)
        relays.append(passed)
    for (axis, other_axis, start), passed in zip(parts, relays):
        for event in passed:
            wait(event)
        _, _, _, dy, dz, _, _ = passed[0]
        second += both(other_axis, dy, dz, start, half)
        sibling(dy, dz, start, half)
    last = []
    for event in second:
        wait(event)
        _, _, _, dy, dz, start, size = event
        last.append(relay(event))
        sibling(dy, dz, start, size)
    for event in last:
        wait(event)
        _, _, _, dy, dz, start, size = event
        sibling(dy, dz, start, size)
    for n, dy, dz, start, size in siblings:
        arrived(n, dy, dz, start, size, True)
    for copy in started:
        copy.wait_send()
    go.wait()


COPIES = 92


def gather_plane(table, number):
    rows, channels = table.shape[0], table.shape[1]
    members = RING * RING * CORES
    return pl.pallas_call(
        functools.partial(gather_kernel, rows, channels),
        out_shape=shape(members, rows, channels, 128),
        in_specs=[pl.BlockSpec(memory_space=pl.ANY)],
        out_specs=pl.BlockSpec(memory_space=pl.ANY),
        scratch_shapes=[
            pltpu.VMEM((rows, channels, 128), BF16),
            pltpu.SemaphoreType.DMA((COPIES,)),
            pltpu.SemaphoreType.DMA((COPIES,)),
            pltpu.SemaphoreType.DMA((2,)),
        ],
        compiler_params=pltpu.CompilerParams(collective_id=number, has_side_effects=True),
        name=f"gather_{number}",
    )(table)


def swap_along_x(parts):
    groups = [[x * RING + z for x in range(RING)] for z in range(RING)]
    return lax.all_to_all(
        parts, "gy", split_axis=0, concat_axis=0, tiled=True, axis_index_groups=groups
    )


def send_halves(table, index, ways, sources, bricks, number):
    channels = table.shape[1]
    gathered = gather_plane(table, number)
    tiles = gathered.shape[0] * gathered.shape[1]
    gathered = gathered.reshape(tiles, channels, 128)
    parts = pl.pallas_call(
        functools.partial(pack, bricks, channels, tiles, ways),
        out_shape=shape(RING, bricks * channels, 512),
        grid_spec=pltpu.PrefetchScalarGridSpec(
            num_scalar_prefetch=1,
            grid=(RING,),
            in_specs=[
                pl.BlockSpec(memory_space=pl.ANY),
                pl.BlockSpec((1, 512), lambda i, index: (0, 0)),
            ],
            out_specs=pl.BlockSpec((1, bricks * channels, 512), lambda i, index: (i, 0, 0)),
            scratch_shapes=[
                pltpu.VMEM((tiles + 1, channels, 128), BF16),
                pltpu.VMEM((bricks * channels, ways * 64), BF16),
                pltpu.VMEM((ways * 64, 512), BF16),
                pltpu.SemaphoreType.DMA,
            ],
        ),
        compiler_params=PARAMS,
        name=f"pack_{number}",
    )(index, gathered, sources)
    return swap_along_x(parts)


def convolve(active, parts, hidden, kernel, bricks, pooled):
    channels = kernel.shape[1]
    outs = [shape(bricks * channels, 512)]
    if pooled:
        outs.append(shape(bricks // 2, channels, 128))
    return pl.pallas_call(
        functools.partial(leave, bricks, channels, pooled),
        out_shape=outs,
        in_specs=whole(6),
        out_specs=whole(len(outs)),
        scratch_shapes=[
            pltpu.VMEM((bricks * channels, 1024), BF16),
            pltpu.VMEM((bricks * channels, 1280), BF16),
            pltpu.VMEM((256, 1152), BF16),
            pltpu.VMEM((3 * channels, 9 * channels), BF16),
            pltpu.VMEM((9 * channels, 640), BF16),
        ],
        compiler_params=PARAMS,
        name=f"convolve_{channels}",
    )(active, parts, hidden, kernel, jnp.asarray(padded_sources()), jnp.asarray(shift_sources()))


def look_up(table, positions):
    hit = positions[:, None] == jnp.arange(table.shape[0], dtype=I32)[None, :]
    return jnp.sum(jnp.where(hit, table[None, :], 0), axis=1)


def owned_rows(links, received, width):
    members, slots = received.shape
    rows = links.reshape(-1)
    me = lax.axis_index("gx") * lax.axis_size("gy") + lax.axis_index("gy")
    remote = rows - width
    is_remote = (remote >= 0) & (remote < members * slots)
    picked = look_up(received.reshape(-1), remote)
    away = jnp.where(is_remote & (picked >= 0), (remote // slots) * width + picked, -1)
    return jnp.where(rows < width, me * width + rows, away)


def rows_here(asked, width):
    x = lax.axis_index("gy") // RING
    owner, row = asked // width, asked % width
    across, along = owner // (RING * RING), owner % (RING * RING)
    here = (asked >= 0) & (along // RING == x)
    members = RING * RING * CORES
    found = (across * RING + along % RING) * width + row
    return jnp.where(here, found, members * width).reshape(-1).astype(I32)


def per_device(
    voxels_fine,
    gain_fine,
    gain_middle,
    gain_coarse,
    kernel_fine,
    kernel_middle,
    kernel_coarse,
    lift_middle,
    lift_coarse,
    links_fine,
    links_middle,
    links_coarse,
    sends_fine,
    sends_middle,
    sends_coarse,
    parents_middle,
    parents_coarse,
    uplinks_middle,
    uplinks_coarse,
):
    members = lax.axis_size("gx") * lax.axis_size("gy")
    bricks = [voxels_fine.shape[0], links_middle.shape[0], links_coarse.shape[0]]
    width = [6 * bricks[0], 6 * bricks[1], 6 * bricks[2], bricks[0], bricks[1]]
    links = [links_fine, links_middle, links_coarse, parents_middle, parents_coarse]
    sends = [
        s.reshape(members, -1)
        for s in (sends_fine, sends_middle, sends_coarse, uplinks_middle, uplinks_coarse)
    ]
    slots = [s.shape[1] for s in sends]
    received = lax.all_to_all(
        jnp.concatenate(sends, axis=1), ("gx", "gy"), split_axis=0, concat_axis=0, tiled=True
    )
    wanted, begin = [], 0
    for n in range(5):
        wanted.append(owned_rows(links[n], received[:, begin : begin + slots[n]], width[n]))
        begin += slots[n]
    counts = [w.shape[0] for w in wanted]
    joined = jnp.concatenate(wanted)
    asked = swap_along_x(jnp.broadcast_to(joined[None], (RING, joined.shape[0])))
    index, begin = [], 0
    for n in range(5):
        index.append(rows_here(asked[:, begin : begin + counts[n]], width[n]))
        begin += counts[n]

    faces, halos, octants = (
        jnp.asarray(face_sources()),
        jnp.asarray(halo_sources()),
        jnp.asarray(octant_sources()),
    )
    channels = [kernel_fine.shape[1], kernel_middle.shape[1], kernel_coarse.shape[1]]
    gains = [g.reshape(-1, 1) for g in (gain_fine, gain_middle, gain_coarse)]

    hidden = voxels_fine.reshape(bricks[0] * channels[0], 512)
    active, table = pl.pallas_call(
        functools.partial(enter_fine, bricks[0], channels[0]),
        out_shape=[shape(bricks[0] * channels[0], 512), shape(3 * bricks[0], channels[0], 128)],
        in_specs=whole(3),
        out_specs=whole(2),
        compiler_params=PARAMS,
        name="enter_0",
    )(hidden, gains[0], faces)
    kernels, lifts = (kernel_fine, kernel_middle, kernel_coarse), (None, lift_middle, lift_coarse)
    outputs = []
    for level in range(3):
        if level:
            parts = send_halves(pooled_table, index[2 + level], 8, octants, bricks[level], 2 * level)
            size = bricks[level] * channels[level]
            hidden, active, table = pl.pallas_call(
                functools.partial(enter_coarser, bricks[level], channels[level - 1], channels[level]),
                out_shape=[
                    shape(size, 512),
                    shape(size, 512),
                    shape(3 * bricks[level], channels[level], 128),
                ],
                in_specs=whole(4),
                out_specs=whole(3),
                compiler_params=PARAMS,
                name=f"enter_{level}",
            )(parts, lifts[level], gains[level], faces)
        parts = send_halves(table, index[level], 26, halos, bricks[level], 2 * level + 1)
        results = convolve(active, parts, hidden, kernels[level], bricks[level], level < 2)
        outputs.append(results[0].reshape(bricks[level], channels[level], 512))
        pooled_table = results[1] if level < 2 else None
    return tuple(outputs)


def solution(mesh):
    split = ("gx", "gy")
    placed = (P(split, None, None),) + (P(),) * 8 + (P(split, None),) * 10
    return jax.shard_map(
        per_device,
        mesh=mesh,
        in_specs=placed,
        out_specs=(P(split, None, None),) * 3,
        check_vma=False,
    )
```

```python
import functools

import jax
import jax.numpy as jnp
import numpy as np
from jax import lax
from jax.experimental import pallas as pl
from jax.experimental.pallas import tpu as pltpu
from jax.sharding import PartitionSpec as P

EPSILON = 1e-06
MESH = pl.DeviceIdType.MESH
BF16, F32, I32 = jnp.bfloat16, jnp.float32, jnp.int32
RING = 4
CORES = 2
VMEM_LIMIT = 60 * 1024 * 1024
DIRECTIONS = [
    (a, b, c) for a in (-1, 0, 1) for b in (-1, 0, 1) for c in (-1, 0, 1) if (a, b, c) != (0, 0, 0)
]


def face_sources():
    ids = np.arange(512).reshape(8, 8, 8)
    layers = [ids[7], ids[0], ids[:, 7], ids[:, 0], ids[:, :, 7], ids[:, :, 0]]
    return np.stack(layers).reshape(1, 384).astype(np.int32)


FACES = [t for t in DIRECTIONS if sum(map(abs, t)) == 1]
FACES = [FACES[0], FACES[5], FACES[1], FACES[4], FACES[2], FACES[3]]
CORNERS = [t for t in DIRECTIONS if sum(map(abs, t)) > 1]


def halo_cells():
    cells = []
    for t in FACES + CORNERS:
        spans = [(0,) if s < 0 else (9,) if s > 0 else range(1, 9) for s in t]
        cells += [(x, y, z) for x in spans[0] for y in spans[1] for z in spans[2]]
    return cells


def corner_sources():
    out = np.full((1, 128), -1, np.int32)
    for n, cell in enumerate(halo_cells()[384:]):
        t = tuple(-1 if v == 0 else 1 if v == 9 else 0 for v in cell)
        lead = next(p for p in range(3) if t[p] != 0)
        u, v = [7 if t[p] < 0 else 0 if t[p] > 0 else cell[p] - 1 for p in range(3) if p != lead]
        out[0, n] = CORNERS.index(t) * 64 + u * 8 + v
    return out


def padded_sources():
    out = np.full((1, 1280), -1, np.int32)
    halo = {cell: n for n, cell in enumerate(halo_cells())}
    for x in range(10):
        for y in range(10):
            for z in range(10):
                if (x, y, z) in halo:
                    source = 512 + halo[x, y, z]
                else:
                    source = (x - 1) * 64 + (y - 1) * 8 + z - 1
                out[0, x * 128 + y * 10 + z] = source
    return out


def shift_sources():
    out = np.zeros((9, 2, 8, 8), np.int32)
    for d in range(9):
        for q in range(2):
            for y in range(8):
                for z in range(8):
                    out[d, q, y, z] = q * 128 + (y + d // 3) * 10 + z + d % 3
    return out.reshape(1, 1152)


def octant_sources():
    out = np.zeros((8, 8, 8), np.int32)
    for x in range(8):
        for y in range(8):
            for z in range(8):
                octant = 4 * (x // 4) + 2 * (y // 4) + z // 4
                out[x, y, z] = octant * 64 + (x % 4) * 16 + (y % 4) * 4 + z % 4
    return out.reshape(1, 512)


def selection(depth, sources):
    rows = lax.broadcasted_iota(I32, (depth, sources.shape[1]), 0)
    return jnp.where(rows == sources, 1.0, 0.0).astype(BF16)


def mm(a, b):
    return jnp.dot(a, b, preferred_element_type=F32)


def as_column(row):
    size = row.shape[1]
    square = lax.broadcasted_iota(I32, (size, size), 0) == lax.broadcasted_iota(I32, (size, size), 1)
    return jnp.sum(jnp.where(square, row, 0.0), axis=1, keepdims=True)


def activate(values, gain):
    mean_sq = jnp.mean(values * values, axis=0, keepdims=True)
    scaled = values * lax.rsqrt(mean_sq + EPSILON) * gain
    return (scaled / (1.0 + jnp.exp(-scaled))).astype(BF16)


def write_faces(bricks, channels, active_ref, sources_ref, table_ref):
    faces = mm(active_ref[...], selection(512, sources_ref[...])).astype(BF16)
    for b in range(bricks):
        for pair in range(3):
            table_ref[3 * b + pair] = faces[
                b * channels : (b + 1) * channels, pair * 128 : (pair + 1) * 128
            ]


def enter_fine(
    bricks,
    channels,
    hidden_ref,
    gain_ref,
    sources_ref,
    *refs,
):
    sends, links = refs[:5], refs[5:10]
    active_ref, table_ref, owed_ref, asked_ref = refs[10:]
    row = 0
    for ref in sends:
        for part in range(ref.shape[1] // 128):
            owed_ref[row : row + 1] = ref[0:1, part * 128 : (part + 1) * 128]
            row += 1
    asked_ref[...] = jnp.zeros(asked_ref.shape, I32)
    row = 0
    for ref in links:
        for b in range(ref.shape[0]):
            lane = row % LINK_ROWS * 32
            asked_ref[row // LINK_ROWS, lane : lane + ref.shape[1]] = ref[b]
            row += 1
    gain = as_column(gain_ref[...])
    for b in range(bricks):
        rows = slice(b * channels, (b + 1) * channels)
        active_ref[rows] = activate(hidden_ref[rows].astype(F32), gain)
    write_faces(bricks, channels, active_ref, sources_ref, table_ref)


def enter_coarser(
    bricks, below, channels, grid_ref, lift_ref, gain_ref, sources_ref, hidden_ref, active_ref, table_ref
):
    gain = as_column(gain_ref[...])
    for b in range(bricks):
        own = slice(b * below, (b + 1) * below)
        rows = slice(b * channels, (b + 1) * channels)
        hidden = lax.dot_general(
            lift_ref[...], grid_ref[own], (((0,), (0,)), ((), ())), preferred_element_type=F32
        ).astype(BF16)
        hidden_ref[rows] = hidden
        active_ref[rows] = activate(hidden.astype(F32), gain)
    write_faces(bricks, channels, active_ref, sources_ref, table_ref)


def tile_of(index_ref, index_row, lane, table_ref):
    row = jnp.clip(index_ref[index_row, lane], 0, 2 * table_ref.shape[0] - 2)
    return table_ref[lax.shift_right_logical(row, 1)], row & 1


def either_half(half, tile, low, want):
    turned = jnp.concatenate([tile[:, 64:], tile[:, :64]], axis=1)
    return jnp.where(half == want, tile, turned)


def pack_halo(bricks, channels, index_ref, dest, base, table_ref, out_ref, gathered_ref, choose):
    lanes = lax.broadcasted_iota(I32, (channels, 128), 1)
    low = lanes < 64
    upper = jnp.where(low, 0, 1)
    order = [DIRECTIONS.index(t) for t in FACES]
    rest = [DIRECTIONS.index(t) for t in CORNERS]

    def brick(b, carry):
        rows = pl.ds(pl.multiple_of(b * channels, channels), channels)
        line = base + b
        index_row, lane = dest * LINK_ROWS + line // LINK_ROWS, line % LINK_ROWS * 32
        for pair in range(3):
            one, first = tile_of(index_ref, index_row, lane + order[2 * pair], table_ref)
            two, second = tile_of(index_ref, index_row, lane + order[2 * pair + 1], table_ref)
            one = either_half(first, one, low, 0)
            two = either_half(second, two, low, 1)
            out_ref[rows, pair * 128 : (pair + 1) * 128] = jnp.where(low, one, two)
        for n, way in enumerate(rest):
            tile, half = tile_of(index_ref, index_row, lane + way, table_ref)
            gathered_ref[rows, n * 128 : (n + 1) * 128] = jnp.where(
                upper == half, tile, jnp.zeros_like(tile)
            )
        return carry

    lax.fori_loop(0, bricks, brick, 0)
    out_ref[:, 384:512] = mm(gathered_ref[...], choose).astype(BF16)


def pack_octants(bricks, channels, index_ref, dest, base, table_ref, out_ref, gathered_ref, choose):
    low = lax.broadcasted_iota(I32, (channels, 128), 1) < 64
    for b in range(bricks):
        rows = slice(b * channels, (b + 1) * channels)
        line = base + b
        index_row, lane = dest * LINK_ROWS + line // LINK_ROWS, line % LINK_ROWS * 32
        for way in range(0, 8, 2):
            one, first = tile_of(index_ref, index_row, lane + way, table_ref)
            two, second = tile_of(index_ref, index_row, lane + way + 1, table_ref)
            one = either_half(first, one, low, 0)
            two = either_half(second, two, low, 1)
            gathered_ref[rows, way * 64 : way * 64 + 128] = jnp.where(low, one, two)
    out_ref[...] = mm(gathered_ref[...], choose).astype(BF16)


def leave(
    bricks,
    channels,
    pooled,
    active_ref,
    halo_ref,
    hidden_ref,
    kernel_ref,
    place_ref,
    shift_ref,
    out_ref,
    *rest,
):
    if pooled:
        table_ref, rest = rest[0], rest[1:]
    source_ref, padded_ref, shifts_ref, weight_ref, moved_ref = rest
    source_ref[:, 0:512] = active_ref[...]
    source_ref[:, 512:1024] = halo_ref[...]
    padded_ref[...] = mm(source_ref[...], selection(1024, place_ref[...])).astype(BF16)
    shifts_ref[...] = selection(256, shift_ref[...])
    for dx in range(3):
        for d in range(9):
            weight_ref[
                dx * channels : (dx + 1) * channels, d * channels : (d + 1) * channels
            ] = kernel_ref[dx * 9 + d]

    def brick(b, carry):
        start = b * channels if isinstance(b, int) else pl.multiple_of(b * channels, channels)
        rows = pl.ds(start, channels)
        planes = jnp.concatenate(
            [padded_ref[rows, pair * 256 : (pair + 1) * 256] for pair in range(5)], axis=0
        )
        moved = mm(planes, shifts_ref[...]).astype(BF16)
        for pair in range(5):
            for d in range(9):
                moved_ref[d * channels : (d + 1) * channels, pair * 128 : (pair + 1) * 128] = moved[
                    pair * channels : (pair + 1) * channels, d * 128 : (d + 1) * 128
                ]
        total = hidden_ref[rows].astype(F32)
        for dx in range(3):
            part = mm(weight_ref[dx * channels : (dx + 1) * channels], moved_ref[...])
            total = total + part[:, dx * 64 : dx * 64 + 512]
        out_ref[rows] = total.astype(BF16)
        return carry

    if bricks > 1:
        lax.fori_loop(0, bricks, brick, 0)
    else:
        brick(0, 0)
    if pooled:
        voxel = lax.broadcasted_iota(I32, (512, 64), 0)
        block = (
            lax.shift_left(lax.shift_right_logical(voxel, 7), 4)
            + lax.shift_left(lax.shift_right_logical(voxel, 4) & 3, 2)
            + (lax.shift_right_logical(voxel, 1) & 3)
        )
        column = lax.broadcasted_iota(I32, (512, 64), 1)
        average = jnp.where(block == column, 0.125, 0.0).astype(BF16)
        blocks = mm(out_ref[...], average).astype(BF16)
        for b in range(bricks):
            table_ref[b // 2, :, (b % 2) * 64 : (b % 2) * 64 + 64] = blocks[
                b * channels : (b + 1) * channels
            ]


def shape(*dims, dtype=BF16):
    return jax.ShapeDtypeStruct(dims, dtype)


def whole(count):
    return [pl.BlockSpec(memory_space=pltpu.VMEM)] * count


PARAMS = pltpu.CompilerParams(vmem_limit_bytes=VMEM_LIMIT)


def place_self():
    across, along = lax.axis_index("gx"), lax.axis_index("gy")
    return across // CORES, across % CORES, along // RING, along % RING


SEND_ROWS = 16
LINK_ROWS = 4
MEMBERS = RING * RING * CORES


def link_constants(steps):
    out = np.zeros((3, 8, 128), np.int32)
    row, position = 0, 0
    for bricks, width, slots in steps:
        for _ in range(bricks):
            lane = row % LINK_ROWS * 32
            out[:, row // LINK_ROWS, lane : lane + 32] = np.array(
                [width, slots.bit_length() - 1, position]
            )[:, None]
            row += 1
        position += slots * MEMBERS * RING
    return out


def resolve(found_ref, links_ref, sends_ref, constants_ref):
    y, core, x, z = place_self()
    own = (y * CORES + core) * RING + z
    sends = sends_ref[...].reshape(MEMBERS * SEND_ROWS, 128).astype(F32).astype(BF16)
    depth = lax.broadcasted_iota(I32, (MEMBERS * SEND_ROWS, 128), 0)
    across = lax.broadcasted_iota(I32, (128, 128), 0)
    for there in range(RING):
        dest = (y * CORES + core) * (RING * RING) + there * RING + z
        for r in range(LINK_ROWS):
            row = links_ref[there, r : r + 1]
            width, log, position = [constants_ref[n, r : r + 1] for n in range(3)]
            remote = row - width
            owner = lax.shift_right_arithmetic(remote, log)
            slot = remote - lax.shift_left(owner, log)
            member = lax.shift_right_arithmetic(owner, 4) * RING + (owner & 3)
            here = (
                (remote >= 0)
                & (owner < MEMBERS * RING)
                & ((lax.shift_right_arithmetic(owner, 2) & 3) == x)
            )
            place = position + lax.shift_left(jnp.full_like(row, dest), log) + slot
            line = jnp.where(here, member * SEND_ROWS + lax.shift_right_logical(place, 7), -1)
            hit = jnp.where(depth == line, 1.0, 0.0).astype(BF16)
            lines = lax.dot_general(
                sends, hit, (((0,), (0,)), ((), ())), preferred_element_type=F32
            )
            picked = jnp.sum(
                jnp.where(across == (place & 127), lines, 0.0), axis=0, keepdims=True
            ).astype(I32)
            found = jnp.where(here & (picked >= 0), member * width + picked, MEMBERS * width)
            mine = (remote < 0) & (jnp.full_like(row, there) == x)
            n = there * LINK_ROWS + r
            found_ref[n : n + 1] = jnp.where(mine, own * width + row, found)


def trade_kernel(bricks, channels, rows, halo, first, base, *refs):
    if first:
        own_ref, sources_ref, sends_ref, links_ref, constants_ref, out_ref, index_ref = refs[:7]
        refs = refs[7:]
    else:
        own_ref, sources_ref, index_ref, out_ref = refs[:4]
        refs = refs[4:]
    all_ref, parts_ref, stage_ref, come_ref, gathered_ref, send_sems, recv_sems, local_sems = refs[:8]
    y, core, x, z = place_self()
    half = channels // 2

    def at(dy, dx, dz, new_core):
        return (((y + dy) % RING) * CORES + new_core, ((x + dx) % RING) * RING + (z + dz) % RING)

    def peer(dy, dz):
        return at(dy, 0, dz, core)

    def block(dy, dz, other=False):
        new_core = 1 - core if other else core
        member = (((y + dy) % RING) * CORES + new_core) * RING + (z + dz) % RING
        return pl.ds(member * rows, rows)

    other_core = at(0, 0, 0, 1 - core)
    along_x = [at(0, k, 0, core) for k in (1, 2, 3)]
    plane = [
        (at(dy, 0, dz, 1 - core if flip else core), dy, dz, flip)
        for dy in range(RING)
        for dz in range(RING)
        for flip in (False, True)
        if (dy, dz, flip) != (0, 0, False)
    ]
    barrier = pltpu.get_barrier_semaphore()
    neighbours = [peer(1, 0), peer(3, 0), peer(0, 1), peer(0, 3), other_core]
    greeted = ([p[0] for p in plane] if first else neighbours) + along_x
    for device in greeted:
        pl.semaphore_signal(barrier, inc=1, device_id=device, device_id_type=MESH)
    all_ref[block(0, 0)] = own_ref[...]
    all_ref[MEMBERS * rows] = jnp.zeros((channels, 128), BF16)
    pl.semaphore_wait(barrier, len(greeted))

    started = []

    def remote(source, target, device):
        n = len(started)
        copy = pltpu.make_async_remote_copy(
            src_ref=source,
            dst_ref=target,
            send_sem=send_sems.at[n],
            recv_sem=recv_sems.at[n],
            device_id=device,
            device_id_type=MESH,
        )
        copy.start()
        started.append(copy)
        return n

    def landed(n, view):
        pltpu.make_async_remote_copy(
            src_ref=view,
            dst_ref=view,
            send_sem=send_sems.at[n],
            recv_sem=recv_sems.at[n],
            device_id=other_core,
            device_id_type=MESH,
        ).wait_recv()

    def send(dy, dz, start, size, device):
        part = pl.ds(start, size)
        source = own_ref.at[:, part] if (dy, dz) == (0, 0) else all_ref.at[block(dy, dz), part]
        return remote(source, all_ref.at[block(dy, dz), part], device)

    siblings = []

    def sibling(dy, dz, start, size):
        siblings.append((send(dy, dz, start, size, other_core), dy, dz, start, size))

    UP, DOWN = 1, 3

    def off(axis, k):
        return (k % RING, 0) if axis == "y" else (0, k % RING)

    def both(axis, dy, dz, start, size):
        events = []
        for step in (UP, DOWN):
            sy, sz = off(axis, step)
            n = send(dy, dz, start, size, peer(sy, sz))
            events.append((n, axis, step, (dy - sy) % RING, (dz - sz) % RING, start, size))
        return events

    def relay(event):
        n, axis, step, dy, dz, start, size = event
        piece = size // 2
        begin = start if step == UP else start + piece
        sy, sz = off(axis, step)
        m = send(dy, dz, begin, piece, peer(sy, sz))
        return (m, axis, step, (dy - sy) % RING, (dz - sz) % RING, begin, piece)

    def wait(event):
        n, _, _, dy, dz, start, size = event
        landed(n, all_ref.at[block(dy, dz), pl.ds(start, size)])

    if first:
        all_sends, all_links, found_ref = refs[8:]
        tables = []
        own_member = (y * CORES + core) * RING + z
        for device, dy, dz, flip in plane:
            n = remote(sends_ref, all_sends.at[own_member], device)
            back = (((y - dy) % RING) * CORES + (1 - core if flip else core)) * RING + (z - dz) % RING
            tables.append((n, all_sends.at[back]))
        for k, device in zip((1, 2, 3), along_x):
            n = remote(links_ref, all_links.at[x], device)
            tables.append((n, all_links.at[(x - k) % RING]))
        all_sends[own_member] = sends_ref[...]
        all_links[x] = links_ref[...]

    axes = [("z", "y", 0), ("y", "z", half)]
    ahead = [both(axis, 0, 0, start, half) for axis, _, start in axes]
    second = []
    for _, axis, start in axes:
        second += both(axis, 0, 0, start, half)
    sibling(0, 0, 0, channels)

    relays = []
    for (_, axis, start), events in zip(axes, ahead):
        passed = []
        for event in events:
            wait(event)
            passed.append(relay(event))
            second += both(axis, event[3], event[4], start, half)
            sibling(event[3], event[4], start, half)
        relays.append(passed)
    for (_, axis, start), passed in zip(axes, relays):
        for event in passed:
            wait(event)
        dy, dz = passed[0][3:5]
        second += both(axis, dy, dz, start, half)
        sibling(dy, dz, start, half)

    def settle():
        last = []
        for event in second:
            wait(event)
            last.append(relay(event))
            sibling(*event[3:])
        for event in last:
            wait(event)
            sibling(*event[3:])
        for n, dy, dz, start, size in siblings:
            landed(n, all_ref.at[block(dy, dz, True), pl.ds(start, size)])

    if first:
        for n, view in tables:
            landed(n, view)
        resolve(found_ref, all_links, all_sends, constants_ref)

    lane = sources_ref[...]
    if halo:
        depth = len(CORNERS) * 128
        at_row = lax.broadcasted_iota(I32, (depth, 128), 0)
        at_row = lax.shift_left(lax.shift_right_logical(at_row, 7), 6) + (at_row & 63)
        choose = jnp.where(at_row == lane, 1.0, 0.0).astype(BF16)
        packer = pack_halo
    else:
        choose = selection(512, lane)
        packer = pack_octants
    settle()
    if first:
        tell = pltpu.make_async_copy(found_ref, index_ref, local_sems.at[0])
        tell.start()
        tell.wait()

    size = bricks * channels
    low, high = pl.ds(0, size // 2), pl.ds(size // 2, size // 2)

    def pack(k):
        packer(
            bricks,
            channels,
            index_ref,
            (x + k) % RING,
            base,
            all_ref,
            parts_ref.at[k],
            gathered_ref,
            choose,
        )

    up, down = along_x[0], along_x[2]
    pack(2)
    pack(1)
    far_up = remote(parts_ref.at[2, low], stage_ref.at[low], up)
    far_down = remote(parts_ref.at[2, high], stage_ref.at[high], down)
    pack(3)
    near_up = [remote(parts_ref.at[1, high], come_ref.at[0, high], up)]
    pack(0)
    near_down = [remote(parts_ref.at[3, low], come_ref.at[1, low], down)]
    landed(far_up, stage_ref.at[low])
    parts_ref[1, low] = (parts_ref[1, low].astype(F32) + stage_ref[low].astype(F32)).astype(BF16)
    landed(far_down, stage_ref.at[high])
    parts_ref[3, high] = (parts_ref[3, high].astype(F32) + stage_ref[high].astype(F32)).astype(BF16)
    near_up.append(remote(parts_ref.at[1, low], come_ref.at[0, low], up))
    near_down.append(remote(parts_ref.at[3, high], come_ref.at[1, high], down))
    landed(near_up[0], come_ref.at[0, high])
    landed(near_down[0], come_ref.at[1, low])
    landed(near_up[1], come_ref.at[0, low])
    landed(near_down[1], come_ref.at[1, high])
    total = parts_ref[0].astype(F32) + come_ref[0].astype(F32) + come_ref[1].astype(F32)
    out_ref[...] = total.astype(BF16)
    for copy in started:
        copy.wait_send()


COPIES = 79 + 34 + 6


def trade(table, number, bricks, sources, halo, base, index=None, tables=None):
    rows, channels = table.shape[0], table.shape[1]
    first = index is None
    size = bricks * channels
    vmem, smem = pl.BlockSpec(memory_space=pltpu.VMEM), pl.BlockSpec(memory_space=pltpu.SMEM)
    outs, out_specs = [shape(size, 512)], [vmem]
    scratch = [
        pltpu.VMEM((MEMBERS * rows + 1, channels, 128), BF16),
        pltpu.VMEM((RING, size, 512), BF16),
        pltpu.VMEM((size, 512), BF16),
        pltpu.VMEM((2, size, 512), BF16),
        pltpu.VMEM((size, len(CORNERS) * 128 if halo else 512), BF16),
        pltpu.SemaphoreType.DMA((COPIES,)),
        pltpu.SemaphoreType.DMA((COPIES,)),
        pltpu.SemaphoreType.DMA((1,)),
    ]
    if first:
        operands, in_specs = (table, sources) + tables, [vmem] * 5
        outs.append(shape(RING * LINK_ROWS, 128, dtype=I32))
        out_specs.append(smem)
        scratch += [
            pltpu.VMEM((MEMBERS, SEND_ROWS, 128), I32),
            pltpu.VMEM((RING, 8, 128), I32),
            pltpu.VMEM((RING * LINK_ROWS, 128), I32),
        ]
    else:
        operands, in_specs = (table, sources, index), [vmem, vmem, smem]
    return pl.pallas_call(
        functools.partial(trade_kernel, bricks, channels, rows, halo, first, base),
        out_shape=outs,
        in_specs=in_specs,
        out_specs=out_specs,
        scratch_shapes=scratch,
        compiler_params=pltpu.CompilerParams(
            collective_id=number, has_side_effects=True, vmem_limit_bytes=VMEM_LIMIT
        ),
        name=f"trade_{number}",
    )(*operands)


def convolve(active, halo, hidden, kernel, bricks, pooled):
    channels = kernel.shape[1]
    outs = [shape(bricks * channels, 512)]
    if pooled:
        outs.append(shape(bricks // 2, channels, 128))
    return pl.pallas_call(
        functools.partial(leave, bricks, channels, pooled),
        out_shape=outs,
        in_specs=whole(6),
        out_specs=whole(len(outs)),
        scratch_shapes=[
            pltpu.VMEM((bricks * channels, 1024), BF16),
            pltpu.VMEM((bricks * channels, 1280), BF16),
            pltpu.VMEM((256, 1152), BF16),
            pltpu.VMEM((3 * channels, 9 * channels), BF16),
            pltpu.VMEM((9 * channels, 640), BF16),
        ],
        compiler_params=PARAMS,
        name=f"convolve_{channels}",
    )(active, halo, hidden, kernel, jnp.asarray(padded_sources()), jnp.asarray(shift_sources()))


def per_device(
    voxels_fine,
    gain_fine,
    gain_middle,
    gain_coarse,
    kernel_fine,
    kernel_middle,
    kernel_coarse,
    lift_middle,
    lift_coarse,
    links_fine,
    links_middle,
    links_coarse,
    sends_fine,
    sends_middle,
    sends_coarse,
    parents_middle,
    parents_coarse,
    uplinks_middle,
    uplinks_coarse,
):
    members = lax.axis_size("gx") * lax.axis_size("gy")
    bricks = [voxels_fine.shape[0], links_middle.shape[0], links_coarse.shape[0]]
    widths = [6 * bricks[0], 6 * bricks[1], 6 * bricks[2], bricks[0], bricks[1]]
    links = [links_fine, links_middle, links_coarse, parents_middle, parents_coarse]
    sends = [sends_fine, sends_middle, sends_coarse, uplinks_middle, uplinks_coarse]
    slots = [s.shape[1] // members for s in sends]
    rows = [t.shape[0] for t in links]
    bases = [sum(rows[:n]) for n in range(5)]
    constants = jnp.asarray(link_constants(tuple(zip(rows, widths, slots))))

    faces, corners, octants = (
        jnp.asarray(face_sources()),
        jnp.asarray(corner_sources()),
        jnp.asarray(octant_sources()),
    )
    channels = [kernel_fine.shape[1], kernel_middle.shape[1], kernel_coarse.shape[1]]
    gains = [g.reshape(1, -1) for g in (gain_fine, gain_middle, gain_coarse)]

    hidden = voxels_fine.reshape(bricks[0] * channels[0], 512)
    active, table, owed, asked = pl.pallas_call(
        functools.partial(enter_fine, bricks[0], channels[0]),
        out_shape=[
            shape(bricks[0] * channels[0], 512),
            shape(3 * bricks[0], channels[0], 128),
            shape(SEND_ROWS, 128, dtype=I32),
            shape(8, 128, dtype=I32),
        ],
        in_specs=whole(13),
        out_specs=whole(4),
        compiler_params=PARAMS,
        name="enter_0",
    )(hidden, gains[0], faces, *sends, *links)
    kernels, lifts = (kernel_fine, kernel_middle, kernel_coarse), (None, lift_middle, lift_coarse)
    outputs = []
    index = None
    for level in range(3):
        if level:
            grid = trade(
                pooled_table, 2 * level, bricks[level], octants, False, bases[2 + level], index
            )[0]
            size = bricks[level] * channels[level]
            hidden, active, table = pl.pallas_call(
                functools.partial(enter_coarser, bricks[level], channels[level - 1], channels[level]),
                out_shape=[
                    shape(size, 512),
                    shape(size, 512),
                    shape(3 * bricks[level], channels[level], 128),
                ],
                in_specs=whole(4),
                out_specs=whole(3),
                compiler_params=PARAMS,
                name=f"enter_{level}",
            )(grid, lifts[level].T, gains[level], faces)
        if level:
            halo = trade(table, 2 * level + 1, bricks[level], corners, True, bases[level], index)[0]
        else:
            halo, index = trade(
                table, 1, bricks[0], corners, True, 0, tables=(owed, asked, constants)
            )
        results = convolve(active, halo, hidden, kernels[level], bricks[level], level < 2)
        outputs.append(results[0].reshape(bricks[level], channels[level], 512))
        pooled_table = results[1] if level < 2 else None
    return tuple(outputs)


def solution(mesh):
    split = ("gx", "gy")
    placed = (P(split, None, None),) + (P(),) * 8 + (P(split, None),) * 10
    return jax.shard_map(
        per_device,
        mesh=mesh,
        in_specs=placed,
        out_specs=(P(split, None, None),) * 3,
        check_vma=False,
    )
```

```python
import functools

import jax
import jax.numpy as jnp
import numpy as np
from jax import lax
from jax.experimental import pallas as pl
from jax.experimental.pallas import tpu as pltpu
from jax.sharding import PartitionSpec as P

EPSILON = 1e-06
MESH = pl.DeviceIdType.MESH
BF16, F32, I32 = jnp.bfloat16, jnp.float32, jnp.int32
RING = 4
CORES = 2
VMEM_LIMIT = 63 * 1024 * 1024
DIRECTIONS = [
    (a, b, c) for a in (-1, 0, 1) for b in (-1, 0, 1) for c in (-1, 0, 1) if (a, b, c) != (0, 0, 0)
]


def face_sources():
    ids = np.arange(512).reshape(8, 8, 8)
    layers = [ids[7], ids[0], ids[:, 7], ids[:, 0], ids[:, :, 7], ids[:, :, 0]]
    return np.stack(layers).reshape(1, 384).astype(np.int32)


FACES = [t for t in DIRECTIONS if sum(map(abs, t)) == 1]
FACES = [FACES[0], FACES[5], FACES[1], FACES[4], FACES[2], FACES[3]]
CORNERS = [t for t in DIRECTIONS if sum(map(abs, t)) > 1]


def halo_cells():
    cells = []
    for t in FACES + CORNERS:
        spans = [(0,) if s < 0 else (9,) if s > 0 else range(1, 9) for s in t]
        cells += [(x, y, z) for x in spans[0] for y in spans[1] for z in spans[2]]
    return cells


def corner_sources():
    out = np.full((1, 128), -1, np.int32)
    for n, cell in enumerate(halo_cells()[384:]):
        t = tuple(-1 if v == 0 else 1 if v == 9 else 0 for v in cell)
        lead = next(p for p in range(3) if t[p] != 0)
        u, v = [7 if t[p] < 0 else 0 if t[p] > 0 else cell[p] - 1 for p in range(3) if p != lead]
        out[0, n] = CORNERS.index(t) * 64 + u * 8 + v
    return out


def padded_sources():
    out = np.full((1, 1280), -1, np.int32)
    halo = {cell: n for n, cell in enumerate(halo_cells())}
    for x in range(10):
        for y in range(10):
            for z in range(10):
                if (x, y, z) in halo:
                    source = 512 + halo[x, y, z]
                else:
                    source = (x - 1) * 64 + (y - 1) * 8 + z - 1
                out[0, x * 128 + y * 10 + z] = source
    return out


def shift_sources():
    out = np.zeros((9, 2, 8, 8), np.int32)
    for d in range(9):
        for q in range(2):
            for y in range(8):
                for z in range(8):
                    out[d, q, y, z] = q * 128 + (y + d // 3) * 10 + z + d % 3
    return out.reshape(1, 1152)


def octant_sources():
    out = np.zeros((8, 8, 8), np.int32)
    for x in range(8):
        for y in range(8):
            for z in range(8):
                octant = 4 * (x // 4) + 2 * (y // 4) + z // 4
                out[x, y, z] = octant * 64 + (x % 4) * 16 + (y % 4) * 4 + z % 4
    return out.reshape(1, 512)


def selection(depth, sources):
    rows = lax.broadcasted_iota(I32, (depth, sources.shape[1]), 0)
    return jnp.where(rows == sources, 1.0, 0.0).astype(BF16)


def mm(a, b):
    return jnp.dot(a, b, preferred_element_type=F32)


def as_column(row):
    size = row.shape[1]
    square = lax.broadcasted_iota(I32, (size, size), 0) == lax.broadcasted_iota(I32, (size, size), 1)
    return jnp.sum(jnp.where(square, row, 0.0), axis=1, keepdims=True)


def activate(values, gain):
    mean_sq = jnp.mean(values * values, axis=0, keepdims=True)
    scaled = values * lax.rsqrt(mean_sq + EPSILON) * gain
    return (scaled / (1.0 + jnp.exp(-scaled))).astype(BF16)


def write_faces(bricks, channels, active_ref, sources_ref, table_ref):
    faces = mm(active_ref[...], selection(512, sources_ref[...])).astype(BF16)
    for b in range(bricks):
        for pair in range(3):
            table_ref[3 * b + pair] = faces[
                b * channels : (b + 1) * channels, pair * 128 : (pair + 1) * 128
            ]


def list_slots(sends, links, owed_ref, asked_ref):
    owed_ref[...] = jnp.zeros(owed_ref.shape, I32)
    for across in range(owed_ref.shape[0]):
        for kind, ref in enumerate(sends):
            part = across * ref.shape[1] // (owed_ref.shape[0] * 128)
            owed_ref[across, kind : kind + 1] = ref[0:1, part * 128 : (part + 1) * 128]
    asked_ref[...] = jnp.zeros(asked_ref.shape, I32)
    row = 0
    for ref in links:
        for b in range(ref.shape[0]):
            lane = row % LINK_ROWS * 32
            asked_ref[row // LINK_ROWS, lane : lane + ref.shape[1]] = ref[b]
            row += 1


def enter_fine(bricks, channels, hidden_ref, gain_ref, sources_ref, active_ref, table_ref):
    gain = as_column(gain_ref[...])
    for b in range(bricks):
        rows = slice(b * channels, (b + 1) * channels)
        active_ref[rows] = activate(hidden_ref[rows].astype(F32), gain)
    write_faces(bricks, channels, active_ref, sources_ref, table_ref)


def enter_coarser(
    bricks, below, channels, turned, grid_ref, lift_ref, gain_ref, sources_ref, hidden_ref, active_ref, table_ref
):
    gain = as_column(gain_ref[...])
    for b in range(bricks):
        own = slice(b * below, (b + 1) * below)
        rows = slice(b * channels, (b + 1) * channels)
        hidden = lax.dot_general(
            lift_ref[...], grid_ref[own], (((0 if turned else 1,), (0,)), ((), ())), preferred_element_type=F32
        ).astype(BF16)
        hidden_ref[rows] = hidden
        active_ref[rows] = activate(hidden.astype(F32), gain)
    write_faces(bricks, channels, active_ref, sources_ref, table_ref)


def tile_of(index_ref, index_row, lane, table_ref):
    row = jnp.clip(index_ref[index_row, lane], 0, 2 * table_ref.shape[0] - 2)
    return table_ref[lax.shift_right_logical(row, 1)], row & 1


def either_half(half, tile, low, want):
    turned = jnp.concatenate([tile[:, 64:], tile[:, :64]], axis=1)
    return jnp.where(half == want, tile, turned)


def pack_halo(bricks, channels, index_ref, dest, base, table_ref, out_ref, gathered_ref, choose):
    lanes = lax.broadcasted_iota(I32, (channels, 128), 1)
    low = lanes < 64
    upper = jnp.where(low, 0, 1)
    order = [DIRECTIONS.index(t) for t in FACES]
    rest = [DIRECTIONS.index(t) for t in CORNERS]

    def brick(b, carry):
        rows = pl.ds(pl.multiple_of(b * channels, channels), channels)
        line = base + b
        index_row, lane = dest * LINK_ROWS + line // LINK_ROWS, line % LINK_ROWS * 32
        for pair in range(3):
            one, first = tile_of(index_ref, index_row, lane + order[2 * pair], table_ref)
            two, second = tile_of(index_ref, index_row, lane + order[2 * pair + 1], table_ref)
            one = either_half(first, one, low, 0)
            two = either_half(second, two, low, 1)
            out_ref[rows, pair * 128 : (pair + 1) * 128] = jnp.where(low, one, two)
        for n, way in enumerate(rest):
            tile, half = tile_of(index_ref, index_row, lane + way, table_ref)
            gathered_ref[rows, n * 128 : (n + 1) * 128] = jnp.where(
                upper == half, tile, jnp.zeros_like(tile)
            )
        return carry

    lax.fori_loop(0, bricks, brick, 0)
    out_ref[:, 384:512] = mm(gathered_ref[...], choose).astype(BF16)


def pack_octants(bricks, channels, index_ref, dest, base, table_ref, out_ref, gathered_ref, choose):
    low = lax.broadcasted_iota(I32, (channels, 128), 1) < 64
    for b in range(bricks):
        rows = slice(b * channels, (b + 1) * channels)
        line = base + b
        index_row, lane = dest * LINK_ROWS + line // LINK_ROWS, line % LINK_ROWS * 32
        for way in range(0, 8, 2):
            one, first = tile_of(index_ref, index_row, lane + way, table_ref)
            two, second = tile_of(index_ref, index_row, lane + way + 1, table_ref)
            one = either_half(first, one, low, 0)
            two = either_half(second, two, low, 1)
            gathered_ref[rows, way * 64 : way * 64 + 128] = jnp.where(low, one, two)
    out_ref[...] = mm(gathered_ref[...], choose).astype(BF16)


def arrange(channels, kernel_ref, weight_ref):
    for dx in range(3):
        for d in range(9):
            weight_ref[
                dx * channels : (dx + 1) * channels, d * channels : (d + 1) * channels
            ] = kernel_ref[dx * 9 + d]


def convolve(
    bricks,
    channels,
    active_ref,
    halo_ref,
    hidden_ref,
    weight_ref,
    place_ref,
    shifts_ref,
    out_ref,
    source_ref,
    padded_ref,
    moved_ref,
):
    source_ref[:, 0:512] = active_ref[...]
    source_ref[:, 512:1024] = halo_ref[...]
    padded_ref[...] = mm(source_ref[...], place_ref[...]).astype(BF16)

    def brick(b, carry):
        start = b * channels if isinstance(b, int) else pl.multiple_of(b * channels, channels)
        rows = pl.ds(start, channels)
        planes = jnp.concatenate(
            [padded_ref[rows, pair * 256 : (pair + 1) * 256] for pair in range(5)], axis=0
        )
        moved = mm(planes, shifts_ref[...]).astype(BF16)
        for pair in range(5):
            for d in range(9):
                moved_ref[d * channels : (d + 1) * channels, pair * 128 : (pair + 1) * 128] = moved[
                    pair * channels : (pair + 1) * channels, d * 128 : (d + 1) * 128
                ]
        parts = mm(weight_ref[...], moved_ref[...])
        total = hidden_ref[rows].astype(F32)
        for dx in range(3):
            total = total + parts[dx * channels : (dx + 1) * channels, dx * 64 : dx * 64 + 512]
        out_ref[rows] = total.astype(BF16)
        return carry

    if bricks > 1:
        lax.fori_loop(0, bricks, brick, 0)
    else:
        brick(0, 0)


def pool(bricks, channels, out_ref, table_ref):
    voxel = lax.broadcasted_iota(I32, (512, 64), 0)
    block = (
        lax.shift_left(lax.shift_right_logical(voxel, 7), 4)
        + lax.shift_left(lax.shift_right_logical(voxel, 4) & 3, 2)
        + (lax.shift_right_logical(voxel, 1) & 3)
    )
    column = lax.broadcasted_iota(I32, (512, 64), 1)
    average = jnp.where(block == column, 0.125, 0.0).astype(BF16)
    blocks = mm(out_ref[...], average).astype(BF16)
    for b in range(bricks):
        table_ref[b // 2, :, (b % 2) * 64 : (b % 2) * 64 + 64] = blocks[
            b * channels : (b + 1) * channels
        ]


def shape(*dims, dtype=BF16):
    return jax.ShapeDtypeStruct(dims, dtype)


def whole(count):
    return [pl.BlockSpec(memory_space=pltpu.VMEM)] * count


PARAMS = pltpu.CompilerParams(vmem_limit_bytes=VMEM_LIMIT)


def place_self():
    across, along = lax.axis_index("gx"), lax.axis_index("gy")
    return across // CORES, across % CORES, along // RING, along % RING


SEND_ROWS = 8
LINK_ROWS = 4
MEMBERS = RING * RING * CORES


def link_constants(steps):
    out = np.zeros((3, 8, 128), np.int32)
    row = 0
    for kind, (bricks, width, slots) in enumerate(steps):
        for _ in range(bricks):
            lane = row % LINK_ROWS * 32
            out[:, row // LINK_ROWS, lane : lane + 32] = np.array(
                [width, slots.bit_length() - 1, kind]
            )[:, None]
            row += 1
    return out


def resolve(found_ref, links_ref, sends_ref, constants_ref):
    y, core, x, z = place_self()
    own = (y * CORES + core) * RING + z
    sends = sends_ref[...].reshape(MEMBERS * SEND_ROWS, 128).astype(F32).astype(BF16)
    depth = lax.broadcasted_iota(I32, (MEMBERS * SEND_ROWS, 128), 0)
    across = lax.broadcasted_iota(I32, (128, 128), 0)
    for there in range(RING):
        dest = (y * CORES + core) * (RING * RING) + there * RING + z
        for r in range(LINK_ROWS):
            row = links_ref[there, r : r + 1]
            width, log, kind = [constants_ref[n, r : r + 1] for n in range(3)]
            remote = row - width
            owner = lax.shift_right_arithmetic(remote, log)
            slot = remote - lax.shift_left(owner, log)
            member = lax.shift_right_arithmetic(owner, 4) * RING + (owner & 3)
            here = (
                (remote >= 0)
                & (owner < MEMBERS * RING)
                & ((lax.shift_right_arithmetic(owner, 2) & 3) == x)
            )
            place = lax.shift_left(jnp.full_like(row, dest), log) + slot
            line = jnp.where(here, member * SEND_ROWS + kind, -1)
            hit = jnp.where(depth == line, 1.0, 0.0).astype(BF16)
            lines = lax.dot_general(
                sends, hit, (((0,), (0,)), ((), ())), preferred_element_type=F32
            )
            picked = jnp.sum(
                jnp.where(across == (place & 127), lines, 0.0), axis=0, keepdims=True
            ).astype(I32)
            found = jnp.where(here & (picked >= 0), member * width + picked, MEMBERS * width)
            mine = (remote < 0) & (jnp.full_like(row, there) == x)
            n = there * LINK_ROWS + r
            found_ref[n : n + 1] = jnp.where(mine, own * width + row, found)


def greet():
    y, core, x, z = place_self()
    barrier = pltpu.get_barrier_semaphore()
    devices = [
        (((y + dy) % RING) * CORES + (1 - core if flip else core), x * RING + (z + dz) % RING)
        for dy in range(RING)
        for dz in range(RING)
        for flip in (False, True)
        if (dy, dz, flip) != (0, 0, False)
    ]
    devices += [(y * CORES + core, ((x + k) % RING) * RING + z) for k in (1, 2, 3)]
    for device in devices:
        pl.semaphore_signal(barrier, inc=1, device_id=device, device_id_type=MESH)
    return len(devices)


def trade(
    bricks,
    channels,
    rows,
    halo,
    base,
    own_ref,
    index_ref,
    out_ref,
    all_ref,
    parts_ref,
    stage_ref,
    come_ref,
    gathered_ref,
    choose_ref,
    send_sems,
    recv_sems,
    tables=None,
    meanwhile=None,
):
    y, core, x, z = place_self()
    half = channels // 2

    def at(dy, dx, dz, new_core):
        return (((y + dy) % RING) * CORES + new_core, ((x + dx) % RING) * RING + (z + dz) % RING)

    def peer(dy, dz):
        return at(dy, 0, dz, core)

    def block(dy, dz, other=False):
        new_core = 1 - core if other else core
        member = (((y + dy) % RING) * CORES + new_core) * RING + (z + dz) % RING
        return pl.ds(member * rows, rows)

    other_core = at(0, 0, 0, 1 - core)
    along_x = [at(0, k, 0, core) for k in (1, 2, 3)]
    plane = [
        (at(dy, 0, dz, 1 - core if flip else core), dy, dz, flip)
        for dy in range(RING)
        for dz in range(RING)
        for flip in (False, True)
        if (dy, dz, flip) != (0, 0, False)
    ]
    all_ref[block(0, 0)] = own_ref[...]
    all_ref[MEMBERS * rows] = jnp.zeros((channels, 128), BF16)

    started = []

    def remote(source, target, device):
        n = len(started)
        copy = pltpu.make_async_remote_copy(
            src_ref=source,
            dst_ref=target,
            send_sem=send_sems.at[n],
            recv_sem=recv_sems.at[n],
            device_id=device,
            device_id_type=MESH,
        )
        copy.start()
        started.append(copy)
        return n

    def landed(n, view):
        pltpu.make_async_remote_copy(
            src_ref=view,
            dst_ref=view,
            send_sem=send_sems.at[n],
            recv_sem=recv_sems.at[n],
            device_id=other_core,
            device_id_type=MESH,
        ).wait_recv()

    def send(dy, dz, start, size, device):
        part = pl.ds(start, size)
        source = own_ref.at[:, part] if (dy, dz) == (0, 0) else all_ref.at[block(dy, dz), part]
        return remote(source, all_ref.at[block(dy, dz), part], device)

    siblings = []

    def sibling(dy, dz, start, size):
        siblings.append((send(dy, dz, start, size, other_core), dy, dz, start, size))

    UP, DOWN = 1, 3

    def off(axis, k):
        return (k % RING, 0) if axis == "y" else (0, k % RING)

    def both(axis, dy, dz, start, size):
        events = []
        for step in (UP, DOWN):
            sy, sz = off(axis, step)
            n = send(dy, dz, start, size, peer(sy, sz))
            events.append((n, axis, step, (dy - sy) % RING, (dz - sz) % RING, start, size))
        return events

    def relay(event):
        n, axis, step, dy, dz, start, size = event
        piece = size // 2
        begin = start if step == UP else start + piece
        sy, sz = off(axis, step)
        m = send(dy, dz, begin, piece, peer(sy, sz))
        return (m, axis, step, (dy - sy) % RING, (dz - sz) % RING, begin, piece)

    def wait(event):
        n, _, _, dy, dz, start, size = event
        landed(n, all_ref.at[block(dy, dz), pl.ds(start, size)])

    arrivals = []
    if tables:
        owed_ref, asked_ref, all_sends, all_links = tables
        own_member = (y * CORES + core) * RING + z
        for device, dy, dz, flip in plane:
            n = remote(owed_ref.at[device[0]], all_sends.at[own_member], device)
            back = (((y - dy) % RING) * CORES + (1 - core if flip else core)) * RING + (z - dz) % RING
            arrivals.append((n, all_sends.at[back]))
        for k, device in zip((1, 2, 3), along_x):
            n = remote(asked_ref, all_links.at[x], device)
            arrivals.append((n, all_links.at[(x - k) % RING]))
        all_sends[own_member] = owed_ref[y * CORES + core]
        all_links[x] = asked_ref[...]

    axes = [("z", "y", 0), ("y", "z", half)]
    ahead = [both(axis, 0, 0, start, half) for axis, _, start in axes]
    second = []
    for _, axis, start in axes:
        second += both(axis, 0, 0, start, half)
    sibling(0, 0, 0, channels)

    relays = []
    for (_, axis, start), events in zip(axes, ahead):
        passed = []
        for event in events:
            wait(event)
            passed.append(relay(event))
            second += both(axis, event[3], event[4], start, half)
            sibling(event[3], event[4], start, half)
        relays.append(passed)
    for (_, axis, start), passed in zip(axes, relays):
        for event in passed:
            wait(event)
        dy, dz = passed[0][3:5]
        second += both(axis, dy, dz, start, half)
        sibling(dy, dz, start, half)

    def settle():
        last = []
        for event in second:
            wait(event)
            last.append(relay(event))
            sibling(*event[3:])
        for event in last:
            wait(event)
            sibling(*event[3:])
        for n, dy, dz, start, size in siblings:
            landed(n, all_ref.at[block(dy, dz, True), pl.ds(start, size)])

    for n, view in arrivals:
        landed(n, view)
    if meanwhile:
        meanwhile()
    settle()
    packer = pack_halo if halo else pack_octants

    size = bricks * channels
    low, high = pl.ds(0, size // 2), pl.ds(size // 2, size // 2)

    def pack(k):
        packer(
            bricks,
            channels,
            index_ref,
            (x + k) % RING,
            base,
            all_ref,
            parts_ref.at[k],
            gathered_ref,
            choose_ref[...],
        )

    up, down = along_x[0], along_x[2]
    pack(2)
    far_up = remote(parts_ref.at[2, low], stage_ref.at[low], up)
    far_down = remote(parts_ref.at[2, high], stage_ref.at[high], down)
    pack(1)
    near_up = [remote(parts_ref.at[1, high], come_ref.at[0, high], up)]
    pack(3)
    near_down = [remote(parts_ref.at[3, low], come_ref.at[1, low], down)]
    landed(far_up, stage_ref.at[low])
    parts_ref[1, low] = (parts_ref[1, low].astype(F32) + stage_ref[low].astype(F32)).astype(BF16)
    landed(far_down, stage_ref.at[high])
    parts_ref[3, high] = (parts_ref[3, high].astype(F32) + stage_ref[high].astype(F32)).astype(BF16)
    near_up.append(remote(parts_ref.at[1, low], come_ref.at[0, low], up))
    near_down.append(remote(parts_ref.at[3, high], come_ref.at[1, high], down))
    pack(0)
    landed(near_up[0], come_ref.at[0, high])
    landed(near_down[0], come_ref.at[1, low])
    landed(near_up[1], come_ref.at[0, low])
    landed(near_down[1], come_ref.at[1, high])
    total = parts_ref[0].astype(F32) + come_ref[0].astype(F32) + come_ref[1].astype(F32)
    out_ref[...] = total.astype(BF16)
    for copy in started:
        copy.wait_send()


COPIES = 79 + 34 + 6


def body_kernel(bricks, channels, *refs):
    (
        voxels, gain0, gain1, gain2, lift1, lift2, constants, faces, corners, octants, places, shifts
    ) = refs[:12]
    sends, links = refs[12:17], refs[17:22]
    kernel0_hbm, kernel1_hbm = refs[22:24]
    out0_hbm, out1_hbm, hidden2, active2, halo2 = refs[24:29]
    (
        owed, asked, all_sends, all_links, found, index,
        active0, hidden1, active1, out0, out1, halo0, halo1, grid1, grid2,
        own0, own1, own2, pooled0, pooled1,
        kernel0, kernel1, weight0, weight1,
        choose_corners, choose_octants, place_matrix, shift_matrix,
        gathered, source, padded, moved,
    ) = refs[29:61]
    buffers = [refs[61 + 4 * n : 65 + 4 * n] for n in range(5)]
    send_sems, recv_sems, local_sems = refs[81:]

    count = greet()
    fetch = [
        pltpu.make_async_copy(kernel0_hbm, kernel0, local_sems.at[0]),
        pltpu.make_async_copy(kernel1_hbm, kernel1, local_sems.at[1]),
    ]
    for copy in fetch:
        copy.start()
    list_slots(sends, links, owed, asked)
    enter_fine(bricks[0], channels[0], voxels, gain0, faces, active0, own0)
    pl.semaphore_wait(pltpu.get_barrier_semaphore(), count)

    def meanwhile():
        resolve(found, all_links, all_sends, constants)
        depth = len(CORNERS) * 128
        at_row = lax.broadcasted_iota(I32, (depth, 128), 0)
        at_row = lax.shift_left(lax.shift_right_logical(at_row, 7), 6) + (at_row & 63)
        choose_corners[...] = jnp.where(at_row == corners[...], 1.0, 0.0).astype(BF16)
        tell = pltpu.make_async_copy(found, index, local_sems.at[2])
        tell.start()
        choose_octants[...] = selection(512, octants[...])
        shift_matrix[...] = selection(256, shifts[...])
        tell.wait()
        for copy in fetch:
            copy.wait()
        arrange(channels[0], kernel0, weight0)

    def step(n, level, halo, base, own, out, **more):
        below = channels[level] if halo else channels[level - 1]
        size = bricks[level] * below
        wide = len(CORNERS) * 128 if halo else 512
        trade(
            bricks[level],
            below,
            own.shape[0],
            halo,
            base,
            own,
            index,
            out,
            *buffers[n],
            gathered.at[pl.ds(0, size), pl.ds(0, wide)],
            choose_corners if halo else choose_octants,
            send_sems.at[n % 2],
            recv_sems.at[n % 2],
            **more,
        )

    def leave(level, active, halo, hidden, weight, out):
        size = bricks[level] * channels[level]
        convolve(
            bricks[level],
            channels[level],
            active,
            halo,
            hidden,
            weight,
            place_matrix,
            shift_matrix,
            out,
            source.at[pl.ds(0, size)],
            padded.at[pl.ds(0, size)],
            moved.at[pl.ds(0, 9 * channels[level])],
        )

    lines = [0, bricks[0], bricks[0] + bricks[1], sum(bricks), sum(bricks) + bricks[1]]
    step(
        0, 0, True, lines[0], own0, halo0, tables=(owed, asked, all_sends, all_links), meanwhile=meanwhile
    )
    place_matrix[...] = selection(1024, places[...])
    leave(0, active0, halo0, voxels, weight0, out0)
    keep0 = pltpu.make_async_copy(out0, out0_hbm, local_sems.at[3])
    keep0.start()
    pool(bricks[0], channels[0], out0, pooled0)
    step(1, 1, False, lines[3], pooled0, grid1, meanwhile=lambda: arrange(channels[1], kernel1, weight1))
    enter_coarser(
        bricks[1], channels[0], channels[1], True, grid1, lift1, gain1, faces, hidden1, active1, own1
    )
    step(2, 1, True, lines[1], own1, halo1)
    leave(1, active1, halo1, hidden1, weight1, out1)
    keep1 = pltpu.make_async_copy(out1, out1_hbm, local_sems.at[4])
    keep1.start()
    pool(bricks[1], channels[1], out1, pooled1)
    step(3, 2, False, lines[4], pooled1, grid2)
    enter_coarser(
        bricks[2], channels[1], channels[2], False, grid2, lift2, gain2, faces, hidden2, active2, own2
    )
    step(4, 2, True, lines[2], own2, halo2)
    keep0.wait()
    keep1.wait()


def last_kernel(
    bricks,
    channels,
    active_ref,
    halo_ref,
    hidden_ref,
    kernel_ref,
    places_ref,
    shifts_ref,
    fine_ref,
    middle_ref,
    fine_out,
    middle_out,
    out_ref,
    place_matrix,
    shift_matrix,
    weight_ref,
    source_ref,
    padded_ref,
    moved_ref,
):
    fine_out[...] = fine_ref[...]
    middle_out[...] = middle_ref[...]
    place_matrix[...] = selection(1024, places_ref[...])
    shift_matrix[...] = selection(256, shifts_ref[...])
    arrange(channels, kernel_ref, weight_ref)
    convolve(
        bricks,
        channels,
        active_ref,
        halo_ref,
        hidden_ref,
        weight_ref,
        place_matrix,
        shift_matrix,
        out_ref,
        source_ref,
        padded_ref,
        moved_ref,
    )


def per_device(
    voxels_fine,
    gain_fine,
    gain_middle,
    gain_coarse,
    kernel_fine,
    kernel_middle,
    kernel_coarse,
    lift_middle,
    lift_coarse,
    links_fine,
    links_middle,
    links_coarse,
    sends_fine,
    sends_middle,
    sends_coarse,
    parents_middle,
    parents_coarse,
    uplinks_middle,
    uplinks_coarse,
):
    members = lax.axis_size("gx") * lax.axis_size("gy")
    bricks = [voxels_fine.shape[0], links_middle.shape[0], links_coarse.shape[0]]
    widths = [6 * bricks[0], 6 * bricks[1], 6 * bricks[2], bricks[0], bricks[1]]
    links = [links_fine, links_middle, links_coarse, parents_middle, parents_coarse]
    sends = [sends_fine, sends_middle, sends_coarse, uplinks_middle, uplinks_coarse]
    slots = [s.shape[1] // members for s in sends]
    rows = [t.shape[0] for t in links]
    constants = jnp.asarray(link_constants(tuple(zip(rows, widths, slots))))

    kernels = (kernel_fine, kernel_middle, kernel_coarse)
    channels = [k.shape[1] for k in kernels]
    sizes = [b * c for b, c in zip(bricks, channels)]
    places, shifts = jnp.asarray(padded_sources()), jnp.asarray(shift_sources())
    gains = [g.reshape(1, -1) for g in (gain_fine, gain_middle, gain_coarse)]
    hidden = voxels_fine.reshape(sizes[0], 512)

    def vmem(*dims, dtype=BF16):
        return pltpu.VMEM(dims, dtype)

    owns = [(3 * b, c, 128) for b, c in zip(bricks, channels)]
    pooled = [(bricks[n] // 2, channels[n], 128) for n in range(2)]
    grids = [bricks[n + 1] * channels[n] for n in range(2)]
    scratch = [
        vmem(2 * RING, SEND_ROWS, 128, dtype=I32),
        vmem(8, 128, dtype=I32),
        vmem(MEMBERS, SEND_ROWS, 128, dtype=I32),
        vmem(RING, 8, 128, dtype=I32),
        vmem(RING * LINK_ROWS, 128, dtype=I32),
        pltpu.SMEM((RING * LINK_ROWS, 128), I32),
        vmem(sizes[0], 512),
        vmem(sizes[1], 512),
        vmem(sizes[1], 512),
        vmem(sizes[0], 512),
        vmem(sizes[1], 512),
        vmem(sizes[0], 512),
        vmem(sizes[1], 512),
        vmem(grids[0], 512),
        vmem(grids[1], 512),
        vmem(*owns[0]),
        vmem(*owns[1]),
        vmem(*owns[2]),
        vmem(*pooled[0]),
        vmem(*pooled[1]),
        vmem(*kernel_fine.shape),
        vmem(*kernel_middle.shape),
        vmem(3 * channels[0], 9 * channels[0]),
        vmem(3 * channels[1], 9 * channels[1]),
        vmem(len(CORNERS) * 128, 128),
        vmem(512, 512),
        vmem(1024, 1280),
        vmem(256, 1152),
        vmem(max(sizes), len(CORNERS) * 128),
        vmem(max(sizes[:2]), 1024),
        vmem(max(sizes[:2]), 1280),
        vmem(9 * channels[1], 640),
    ]
    for table, size in zip(
        (owns[0], pooled[0], owns[1], pooled[1], owns[2]),
        (sizes[0], grids[0], sizes[1], grids[1], sizes[2]),
    ):
        scratch += [
            vmem(MEMBERS * table[0] + 1, table[1], 128),
            vmem(RING, size, 512),
            vmem(size, 512),
            vmem(2, size, 512),
        ]
    scratch += [
        pltpu.SemaphoreType.DMA((2, COPIES)),
        pltpu.SemaphoreType.DMA((2, COPIES)),
        pltpu.SemaphoreType.DMA((5,)),
    ]
    anywhere = pl.BlockSpec(memory_space=pl.ANY)
    fine, middle, hidden, active, halo = pl.pallas_call(
        functools.partial(body_kernel, bricks, channels),
        out_shape=[shape(sizes[0], 512), shape(sizes[1], 512)] + [shape(sizes[2], 512)] * 3,
        in_specs=whole(22) + [anywhere] * 2,
        out_specs=[anywhere] * 2 + whole(3),
        scratch_shapes=scratch,
        compiler_params=pltpu.CompilerParams(
            collective_id=0, has_side_effects=True, vmem_limit_bytes=VMEM_LIMIT
        ),
        name="levels",
    )(
        hidden,
        *gains,
        lift_middle.T,
        lift_coarse,
        constants,
        jnp.asarray(face_sources()),
        jnp.asarray(corner_sources()),
        jnp.asarray(octant_sources()),
        places,
        shifts,
        *sends,
        *links,
        kernel_fine,
        kernel_middle,
    )
    outputs = pl.pallas_call(
        functools.partial(last_kernel, bricks[2], channels[2]),
        out_shape=[shape(size, 512) for size in sizes],
        in_specs=whole(8),
        out_specs=whole(3),
        scratch_shapes=[
            vmem(1024, 1280),
            vmem(256, 1152),
            vmem(3 * channels[2], 9 * channels[2]),
            vmem(sizes[2], 1024),
            vmem(sizes[2], 1280),
            vmem(9 * channels[2], 640),
        ],
        compiler_params=PARAMS,
        name="last",
    )(active, halo, hidden, kernel_coarse, places, shifts, fine, middle)
    return tuple(
        out.reshape(b, c, 512) for out, b, c in zip(outputs, bricks, channels)
    )


def solution(mesh):
    split = ("gx", "gy")
    placed = (P(split, None, None),) + (P(),) * 8 + (P(split, None),) * 10
    return jax.shard_map(
        per_device,
        mesh=mesh,
        in_specs=placed,
        out_specs=(P(split, None, None),) * 3,
        check_vma=False,
    )
```

```python
import functools

import jax
import jax.numpy as jnp
import numpy as np
from jax import lax
from jax.experimental import pallas as pl
from jax.experimental.pallas import tpu as pltpu
from jax.sharding import PartitionSpec as P

EPSILON = 1e-06
MESH = pl.DeviceIdType.MESH
BF16, F32, I32 = jnp.bfloat16, jnp.float32, jnp.int32
RING = 4
CORES = 2
VMEM_LIMIT = 63 * 1024 * 1024
CHUNKS = (1, 1, 1, 1, 1)
DIRECTIONS = [
    (a, b, c) for a in (-1, 0, 1) for b in (-1, 0, 1) for c in (-1, 0, 1) if (a, b, c) != (0, 0, 0)
]


def face_sources():
    ids = np.arange(512).reshape(8, 8, 8)
    layers = [ids[7], ids[0], ids[:, 7], ids[:, 0], ids[:, :, 7], ids[:, :, 0]]
    return np.stack(layers).reshape(1, 384).astype(np.int32)


FACES = [t for t in DIRECTIONS if sum(map(abs, t)) == 1]
FACES = [FACES[0], FACES[5], FACES[1], FACES[4], FACES[2], FACES[3]]
CORNERS = [t for t in DIRECTIONS if sum(map(abs, t)) > 1]


def halo_cells():
    cells = []
    for t in FACES + CORNERS:
        spans = [(0,) if s < 0 else (9,) if s > 0 else range(1, 9) for s in t]
        cells += [(x, y, z) for x in spans[0] for y in spans[1] for z in spans[2]]
    return cells


def slab_lanes(t):
    lead = next(p for p in range(3) if t[p] != 0)
    spans = [(0,) if s < 0 else (9,) if s > 0 else range(1, 9) for s in t]
    found = []
    for cell in [(x, y, z) for x in spans[0] for y in spans[1] for z in spans[2]]:
        u, v = [7 if t[p] < 0 else 0 if t[p] > 0 else cell[p] - 1 for p in range(3) if p != lead]
        found.append((u * 8 + v, cell))
    return found


def corner_groups():
    groups = []
    for t in CORNERS:
        mine = {lane for lane, _ in slab_lanes(t)}
        for group, taken in groups:
            if not mine & taken:
                group.append(t)
                taken |= mine
                break
        else:
            groups.append(([t], set(mine)))
    return [group for group, _ in groups]


GROUPS = corner_groups()
KINDS = sorted({tuple(sorted(lane for lane, _ in slab_lanes(t))) for t in CORNERS})


def kind_of(t):
    return KINDS.index(tuple(sorted(lane for lane, _ in slab_lanes(t))))


def kind_masks():
    out = np.zeros((2 * len(KINDS), 16, 128), np.int32)
    for n, lanes in enumerate(KINDS):
        for half in range(2):
            out[2 * n + half][:, [64 * half + lane for lane in lanes]] = 1
    return out


def corner_sources():
    out = np.full((1, 128), -1, np.int32)
    cells = halo_cells()[384:]
    for n, group in enumerate(GROUPS):
        for t in group:
            for lane, cell in slab_lanes(t):
                out[0, cells.index(cell)] = n * 64 + lane
    return out


def padded_sources():
    out = np.full((1, 1280), -1, np.int32)
    halo = {cell: n for n, cell in enumerate(halo_cells())}
    for x in range(10):
        for y in range(10):
            for z in range(10):
                if (x, y, z) in halo:
                    source = 512 + halo[x, y, z]
                else:
                    source = (x - 1) * 64 + (y - 1) * 8 + z - 1
                out[0, x * 128 + y * 10 + z] = source
    return out


def shift_sources():
    out = np.zeros((9, 2, 8, 8), np.int32)
    for d in range(9):
        for q in range(2):
            for y in range(8):
                for z in range(8):
                    out[d, q, y, z] = q * 128 + (y + d // 3) * 10 + z + d % 3
    return out.reshape(1, 1152)


def octant_sources():
    out = np.zeros((8, 8, 8), np.int32)
    for x in range(8):
        for y in range(8):
            for z in range(8):
                octant = 4 * (x // 4) + 2 * (y // 4) + z // 4
                out[x, y, z] = octant * 64 + (x % 4) * 16 + (y % 4) * 4 + z % 4
    return out.reshape(1, 512)


def selection(depth, sources):
    rows = lax.broadcasted_iota(I32, (depth, sources.shape[1]), 0)
    return jnp.where(rows == sources, 1.0, 0.0).astype(BF16)


def mm(a, b):
    return jnp.dot(a, b, preferred_element_type=F32)


def as_column(row):
    size = row.shape[1]
    square = lax.broadcasted_iota(I32, (size, size), 0) == lax.broadcasted_iota(I32, (size, size), 1)
    return jnp.sum(jnp.where(square, row, 0.0), axis=1, keepdims=True)


def activate(values, gain):
    mean_sq = jnp.mean(values * values, axis=0, keepdims=True)
    scaled = values * lax.rsqrt(mean_sq + EPSILON) * gain
    return (scaled / (1.0 + jnp.exp(-scaled))).astype(BF16)


def write_faces(bricks, channels, active_ref, sources_ref, table_ref):
    faces = mm(active_ref[...], selection(512, sources_ref[...])).astype(BF16)
    for b in range(bricks):
        for pair in range(3):
            table_ref[3 * b + pair] = faces[
                b * channels : (b + 1) * channels, pair * 128 : (pair + 1) * 128
            ]


def list_slots(sends, links, owed_ref, asked_ref):
    owed_ref[...] = jnp.zeros(owed_ref.shape, I32)
    for across in range(owed_ref.shape[0]):
        for kind, ref in enumerate(sends):
            part = across * ref.shape[1] // (owed_ref.shape[0] * 128)
            owed_ref[across, kind : kind + 1] = ref[0:1, part * 128 : (part + 1) * 128]
    asked_ref[...] = jnp.zeros(asked_ref.shape, I32)
    row = 0
    for ref in links:
        for b in range(ref.shape[0]):
            lane = row % LINK_ROWS * 32
            asked_ref[row // LINK_ROWS, lane : lane + ref.shape[1]] = ref[b]
            row += 1


def enter_fine(bricks, channels, hidden_ref, gain_ref, sources_ref, active_ref, table_ref):
    gain = as_column(gain_ref[...])
    for b in range(bricks):
        rows = slice(b * channels, (b + 1) * channels)
        active_ref[rows] = activate(hidden_ref[rows].astype(F32), gain)
    write_faces(bricks, channels, active_ref, sources_ref, table_ref)


def enter_coarser(
    bricks, below, channels, turned, grid_ref, lift_ref, gain_ref, sources_ref, hidden_ref, active_ref, table_ref
):
    gain = as_column(gain_ref[...])
    for b in range(bricks):
        own = slice(b * below, (b + 1) * below)
        rows = slice(b * channels, (b + 1) * channels)
        hidden = lax.dot_general(
            lift_ref[...], grid_ref[own], (((0 if turned else 1,), (0,)), ((), ())), preferred_element_type=F32
        ).astype(BF16)
        hidden_ref[rows] = hidden
        active_ref[rows] = activate(hidden.astype(F32), gain)
    write_faces(bricks, channels, active_ref, sources_ref, table_ref)


LOW, HIGH, NONE = 0, 1, 2


def write_masks(masks_ref, kinds_ref):
    masks_ref[3:] = kinds_ref[...].astype(F32).astype(BF16)
    lanes = lax.broadcasted_iota(I32, (16, 128), 1)
    masks_ref[LOW] = jnp.where(lanes < 64, 1.0, 0.0).astype(BF16)
    masks_ref[HIGH] = jnp.where(lanes < 64, 0.0, 1.0).astype(BF16)
    masks_ref[NONE] = jnp.zeros((16, 128), BF16)


def tile_of(index_ref, index_row, lane, table_ref, part):
    row = jnp.clip(index_ref[index_row, lane], 0, 2 * table_ref.shape[0] - 2)
    return table_ref[lax.shift_right_logical(row, 1), part], row & 1


def masked(tile, mask):
    channels = tile.shape[0]
    return (tile.reshape(channels // 16, 16, 128) * mask[None]).reshape(channels, 128)


def turn(tile):
    return jnp.concatenate([tile[:, 64:], tile[:, :64]], axis=1)


def side_by_side(one, first, two, second, masks_ref):
    low = masked(one, masks_ref[2 * first]) + masked(turn(one), masks_ref[2 - 2 * first])
    high = masked(two, masks_ref[2 - second]) + masked(turn(two), masks_ref[1 + second])
    return low + high


def pack_halo(bricks, part, index_ref, dest, base, table_ref, out_ref, gathered_ref, choose, masks_ref):
    channels = part.size
    order = [DIRECTIONS.index(t) for t in FACES]

    def brick(b, carry):
        start = b * channels if isinstance(b, int) else pl.multiple_of(b * channels, channels)
        rows = pl.ds(start, channels)
        line = base + b
        index_row, lane = dest * LINK_ROWS + line // LINK_ROWS, line % LINK_ROWS * 32
        for pair in range(3):
            one, first = tile_of(index_ref, index_row, lane + order[2 * pair], table_ref, part)
            two, second = tile_of(index_ref, index_row, lane + order[2 * pair + 1], table_ref, part)
            out_ref[rows, pair * 128 : (pair + 1) * 128] = side_by_side(
                one, first, two, second, masks_ref
            )
        for n, group in enumerate(GROUPS):
            shared = None
            for t in group:
                way = lane + DIRECTIONS.index(t)
                tile, half = tile_of(index_ref, index_row, way, table_ref, part)
                piece = masked(tile, masks_ref[3 + 2 * kind_of(t) + half])
                shared = piece if shared is None else shared + piece
            gathered_ref[rows, n * 128 : (n + 1) * 128] = shared
        return carry

    if bricks > 1:
        lax.fori_loop(0, bricks, brick, 0)
    else:
        brick(0, 0)
    out_ref[:, 384:512] = mm(gathered_ref[...], choose).astype(BF16)


def pack_octants(bricks, part, index_ref, dest, base, table_ref, out_ref, gathered_ref, choose, masks_ref):
    channels = part.size
    for b in range(bricks):
        rows = slice(b * channels, (b + 1) * channels)
        line = base + b
        index_row, lane = dest * LINK_ROWS + line // LINK_ROWS, line % LINK_ROWS * 32
        for way in range(0, 8, 2):
            one, first = tile_of(index_ref, index_row, lane + way, table_ref, part)
            two, second = tile_of(index_ref, index_row, lane + way + 1, table_ref, part)
            gathered_ref[rows, way * 64 : way * 64 + 128] = side_by_side(
                one, first, two, second, masks_ref
            )
    out_ref[...] = mm(gathered_ref[...], choose).astype(BF16)


def arrange(channels, kernel_ref, weight_ref):
    for dx in range(3):
        for d in range(9):
            weight_ref[
                dx * channels : (dx + 1) * channels, d * channels : (d + 1) * channels
            ] = kernel_ref[dx * 9 + d]


def convolve(
    bricks,
    channels,
    active_ref,
    halo_ref,
    hidden_ref,
    weight_ref,
    place_ref,
    shifts_ref,
    out_ref,
    source_ref,
    padded_ref,
    moved_ref,
):
    source_ref[:, 0:512] = active_ref[...]
    source_ref[:, 512:1024] = halo_ref[...]
    padded_ref[...] = mm(source_ref[...], place_ref[...]).astype(BF16)

    def brick(b, carry):
        start = b * channels if isinstance(b, int) else pl.multiple_of(b * channels, channels)
        rows = pl.ds(start, channels)
        planes = jnp.concatenate(
            [padded_ref[rows, pair * 256 : (pair + 1) * 256] for pair in range(5)], axis=0
        )
        moved = mm(planes, shifts_ref[...]).astype(BF16)
        for pair in range(5):
            for d in range(9):
                moved_ref[d * channels : (d + 1) * channels, pair * 128 : (pair + 1) * 128] = moved[
                    pair * channels : (pair + 1) * channels, d * 128 : (d + 1) * 128
                ]
        parts = mm(weight_ref[...], moved_ref[...])
        total = hidden_ref[rows].astype(F32)
        for dx in range(3):
            total = total + parts[dx * channels : (dx + 1) * channels, dx * 64 : dx * 64 + 512]
        out_ref[rows] = total.astype(BF16)
        return carry

    if bricks > 1:
        lax.fori_loop(0, bricks, brick, 0)
    else:
        brick(0, 0)


def pool(bricks, channels, out_ref, table_ref):
    voxel = lax.broadcasted_iota(I32, (512, 64), 0)
    block = (
        lax.shift_left(lax.shift_right_logical(voxel, 7), 4)
        + lax.shift_left(lax.shift_right_logical(voxel, 4) & 3, 2)
        + (lax.shift_right_logical(voxel, 1) & 3)
    )
    column = lax.broadcasted_iota(I32, (512, 64), 1)
    average = jnp.where(block == column, 0.125, 0.0).astype(BF16)
    blocks = mm(out_ref[...], average).astype(BF16)
    for b in range(bricks):
        table_ref[b // 2, :, (b % 2) * 64 : (b % 2) * 64 + 64] = blocks[
            b * channels : (b + 1) * channels
        ]


def shape(*dims, dtype=BF16):
    return jax.ShapeDtypeStruct(dims, dtype)


def whole(count):
    return [pl.BlockSpec(memory_space=pltpu.VMEM)] * count


PARAMS = pltpu.CompilerParams(vmem_limit_bytes=VMEM_LIMIT)


def place_self():
    across, along = lax.axis_index("gx"), lax.axis_index("gy")
    return across // CORES, across % CORES, along // RING, along % RING


SEND_ROWS = 8
LINK_ROWS = 4
MEMBERS = RING * RING * CORES


def link_constants(steps):
    out = np.zeros((3, 8, 128), np.int32)
    row = 0
    for kind, (bricks, width, slots) in enumerate(steps):
        for _ in range(bricks):
            lane = row % LINK_ROWS * 32
            out[:, row // LINK_ROWS, lane : lane + 32] = np.array(
                [width, slots.bit_length() - 1, kind]
            )[:, None]
            row += 1
    return out


def resolve(found_ref, links_ref, sends_ref, constants_ref):
    y, core, x, z = place_self()
    own = (y * CORES + core) * RING + z
    sends = sends_ref[...].reshape(MEMBERS * SEND_ROWS, 128).astype(F32).astype(BF16)
    depth = lax.broadcasted_iota(I32, (MEMBERS * SEND_ROWS, 128), 0)
    across = lax.broadcasted_iota(I32, (128, 128), 0)
    for there in range(RING):
        dest = (y * CORES + core) * (RING * RING) + there * RING + z
        for r in range(LINK_ROWS):
            row = links_ref[there, r : r + 1]
            width, log, kind = [constants_ref[n, r : r + 1] for n in range(3)]
            remote = row - width
            owner = lax.shift_right_arithmetic(remote, log)
            slot = remote - lax.shift_left(owner, log)
            member = lax.shift_right_arithmetic(owner, 4) * RING + (owner & 3)
            here = (
                (remote >= 0)
                & (owner < MEMBERS * RING)
                & ((lax.shift_right_arithmetic(owner, 2) & 3) == x)
            )
            place = lax.shift_left(jnp.full_like(row, dest), log) + slot
            line = jnp.where(here, member * SEND_ROWS + kind, -1)
            hit = jnp.where(depth == line, 1.0, 0.0).astype(BF16)
            lines = lax.dot_general(
                sends, hit, (((0,), (0,)), ((), ())), preferred_element_type=F32
            )
            picked = jnp.sum(
                jnp.where(across == (place & 127), lines, 0.0), axis=0, keepdims=True
            ).astype(I32)
            found = jnp.where(here & (picked >= 0), member * width + picked, MEMBERS * width)
            mine = (remote < 0) & (jnp.full_like(row, there) == x)
            n = there * LINK_ROWS + r
            found_ref[n : n + 1] = jnp.where(mine, own * width + row, found)


def greet():
    y, core, x, z = place_self()
    barrier = pltpu.get_barrier_semaphore()
    devices = [
        (((y + dy) % RING) * CORES + (1 - core if flip else core), x * RING + (z + dz) % RING)
        for dy in range(RING)
        for dz in range(RING)
        for flip in (False, True)
        if (dy, dz, flip) != (0, 0, False)
    ]
    devices += [(y * CORES + core, ((x + k) % RING) * RING + z) for k in (1, 2, 3)]
    for device in devices:
        pl.semaphore_signal(barrier, inc=1, device_id=device, device_id_type=MESH)
    return len(devices)


def trade(
    bricks,
    channels,
    rows,
    halo,
    base,
    own_ref,
    index_ref,
    out_ref,
    all_ref,
    parts_ref,
    stage_ref,
    come_ref,
    gathered_ref,
    choose_ref,
    masks_ref,
    send_sems,
    recv_sems,
    chunks,
    tables=None,
    meanwhile=None,
):
    y, core, x, z = place_self()
    width = channels // chunks
    half = width // 2

    def at(dy, dx, dz, new_core):
        return (((y + dy) % RING) * CORES + new_core, ((x + dx) % RING) * RING + (z + dz) % RING)

    def peer(dy, dz):
        return at(dy, 0, dz, core)

    def block(dy, dz, other=False, first_row=0, count=rows):
        new_core = 1 - core if other else core
        member = (((y + dy) % RING) * CORES + new_core) * RING + (z + dz) % RING
        return pl.ds(member * rows + first_row, count)

    other_core = at(0, 0, 0, 1 - core)
    along_x = [at(0, k, 0, core) for k in (1, 2, 3)]
    plane = [
        (at(dy, 0, dz, 1 - core if flip else core), dy, dz, flip)
        for dy in range(RING)
        for dz in range(RING)
        for flip in (False, True)
        if (dy, dz, flip) != (0, 0, False)
    ]
    all_ref[block(0, 0)] = own_ref[...]
    all_ref[MEMBERS * rows] = jnp.zeros((channels, 128), BF16)

    started = []

    def remote(source, target, device):
        n = len(started)
        copy = pltpu.make_async_remote_copy(
            src_ref=source,
            dst_ref=target,
            send_sem=send_sems.at[n],
            recv_sem=recv_sems.at[n],
            device_id=device,
            device_id_type=MESH,
        )
        copy.start()
        started.append(copy)
        return n

    def landed(n, view):
        pltpu.make_async_remote_copy(
            src_ref=view,
            dst_ref=view,
            send_sem=send_sems.at[n],
            recv_sem=recv_sems.at[n],
            device_id=other_core,
            device_id_type=MESH,
        ).wait_recv()

    def view(dy, dz, region, other=False):
        row, count, start, size = region
        return all_ref.at[block(dy, dz, other, row, count), pl.ds(start, size)]

    def send(dy, dz, region, device):
        row, count, start, size = region
        source = view(dy, dz, region)
        if (dy, dz) == (0, 0):
            source = own_ref.at[pl.ds(row, count), pl.ds(start, size)]
        return remote(source, view(dy, dz, region), device)

    UP, DOWN = 1, 3

    def off(axis, k):
        return (k % RING, 0) if axis == "y" else (0, k % RING)

    def both(axis, dy, dz, region):
        events = []
        for step in (UP, DOWN):
            sy, sz = off(axis, step)
            n = send(dy, dz, region, peer(sy, sz))
            events.append((n, axis, step, (dy - sy) % RING, (dz - sz) % RING, region))
        return events

    def relay(event):
        n, axis, step, dy, dz, (row, count, start, size) = event
        if size // 2 >= 16:
            begin = start if step == UP else start + size // 2
            region = (row, count, begin, size // 2)
        else:
            region = (row if step == UP else row + count // 2, count // 2, start, size)
        sy, sz = off(axis, step)
        m = send(dy, dz, region, peer(sy, sz))
        return (m, axis, step, (dy - sy) % RING, (dz - sz) % RING, region)

    def wait(event):
        n, _, _, dy, dz, region = event
        landed(n, view(dy, dz, region))

    class Gather:
        def __init__(self, chunk):
            start = chunk * width
            self.whole = (0, rows, start, width)
            self.axes = [("z", "y", (0, rows, start, half)), ("y", "z", (0, rows, start + half, half))]
            self.second, self.siblings, self.last = [], [], []

        def sibling(self, dy, dz, region):
            self.siblings.append((send(dy, dz, region, other_core), dy, dz, region))

        def begin(self):
            self.ahead = [both(axis, 0, 0, region) for axis, _, region in self.axes]
            for _, axis, region in self.axes:
                self.second += both(axis, 0, 0, region)
            self.sibling(0, 0, self.whole)

        def neighbours(self):
            relays = []
            for (_, axis, region), events in zip(self.axes, self.ahead):
                passed = []
                for event in events:
                    wait(event)
                    passed.append(relay(event))
                    self.second += both(axis, event[3], event[4], region)
                    self.sibling(event[3], event[4], region)
                relays.append(passed)
            for (_, axis, region), passed in zip(self.axes, relays):
                for event in passed:
                    wait(event)
                dy, dz = passed[0][3:5]
                self.second += both(axis, dy, dz, region)
                self.sibling(dy, dz, region)

        def forward(self, count):
            for event in self.second[:count]:
                wait(event)
                self.last.append(relay(event))
                self.sibling(*event[3:])
            self.second = self.second[count:]

        def finish(self):
            self.forward(len(self.second))
            for event in self.last:
                wait(event)
                self.sibling(*event[3:])
            for n, dy, dz, region in self.siblings:
                landed(n, view(dy, dz, region, True))

    size = bricks * width
    low, high = pl.ds(0, size // 2), pl.ds(size // 2, size // 2)
    packer = pack_halo if halo else pack_octants
    up, down = along_x[0], along_x[2]

    class Exchange:
        def __init__(self, chunk):
            self.chunk = chunk

        def at(self, ref, *place):
            return ref.at[(*place[:-1], self.chunk, place[-1])]

        def pack(self, k):
            packer(
                bricks,
                pl.ds(self.chunk * width, width),
                index_ref,
                (x + k) % RING,
                base,
                all_ref,
                parts_ref.at[k, self.chunk],
                gathered_ref,
                choose_ref[...],
                masks_ref,
            )

        def far(self):
            self.pack(2)
            self.far_up = remote(self.at(parts_ref, 2, low), self.at(stage_ref, low), up)
            self.far_down = remote(self.at(parts_ref, 2, high), self.at(stage_ref, high), down)

        def near_up(self):
            self.pack(1)
            self.ups = [remote(self.at(parts_ref, 1, high), self.at(come_ref, 0, high), up)]

        def near_down(self):
            self.pack(3)
            self.downs = [remote(self.at(parts_ref, 3, low), self.at(come_ref, 1, low), down)]

        def add(self, k, rows):
            place = (k, self.chunk, rows)
            more = stage_ref[self.chunk, rows].astype(F32)
            parts_ref[place] = (parts_ref[place].astype(F32) + more).astype(BF16)

        def passed_on(self):
            landed(self.far_up, self.at(stage_ref, low))
            self.add(1, low)
            self.ups.append(remote(self.at(parts_ref, 1, low), self.at(come_ref, 0, low), up))
            landed(self.far_down, self.at(stage_ref, high))
            self.add(3, high)
            self.downs.append(remote(self.at(parts_ref, 3, high), self.at(come_ref, 1, high), down))

        def finish(self):
            landed(self.ups[0], self.at(come_ref, 0, high))
            landed(self.downs[0], self.at(come_ref, 1, low))
            landed(self.ups[1], self.at(come_ref, 0, low))
            landed(self.downs[1], self.at(come_ref, 1, high))
            for b in range(bricks):
                part = pl.ds(b * width, width)
                total = (
                    parts_ref[0, self.chunk, part].astype(F32)
                    + come_ref[0, self.chunk, part].astype(F32)
                    + come_ref[1, self.chunk, part].astype(F32)
                )
                begin = b * channels + self.chunk * width
                out_ref[begin : begin + width] = total.astype(BF16)

    arrivals = []
    if tables:
        owed_ref, asked_ref, all_sends, all_links = tables
        own_member = (y * CORES + core) * RING + z
        for device, dy, dz, flip in plane:
            n = remote(owed_ref.at[device[0]], all_sends.at[own_member], device)
            back = (((y - dy) % RING) * CORES + (1 - core if flip else core)) * RING + (z - dz) % RING
            arrivals.append((n, all_sends.at[back]))
        for k, device in zip((1, 2, 3), along_x):
            n = remote(asked_ref, all_links.at[x], device)
            arrivals.append((n, all_links.at[(x - k) % RING]))
        all_sends[own_member] = owed_ref[y * CORES + core]
        all_links[x] = asked_ref[...]

    gathers = [Gather(chunk) for chunk in range(chunks)]
    exchanges = [Exchange(chunk) for chunk in range(chunks)]
    gathers[0].begin()
    gathers[0].neighbours()
    if chunks > 1:
        gathers[1].begin()
    for n, arrival in arrivals:
        landed(n, arrival)
    if meanwhile:
        meanwhile()
    gathers[0].forward(len(gathers[0].second))
    if chunks > 1:
        gathers[1].neighbours()
    gathers[0].finish()

    def tick(count):
        if chunks > 1:
            gathers[1].forward(count)

    exchanges[0].far()
    tick(4)
    exchanges[0].near_up()
    tick(4)
    exchanges[0].near_down()
    tick(4)
    exchanges[0].passed_on()
    tick(4)
    exchanges[0].pack(0)
    if chunks > 1:
        gathers[1].finish()
        exchanges[1].far()
        exchanges[1].near_up()
        exchanges[1].near_down()
        exchanges[1].passed_on()
        exchanges[1].pack(0)
    for exchange in exchanges:
        exchange.finish()
    for copy in started:
        copy.wait_send()


COPIES = 2 * (79 + 6) + 34


def body_kernel(bricks, channels, *refs):
    (
        voxels, gain0, gain1, gain2, lift1, lift2, constants, faces, corners, octants, places, shifts,
        kinds,
    ) = refs[:13]
    sends, links = refs[13:18], refs[18:23]
    kernel0_hbm, kernel1_hbm, kernel2_hbm = refs[23:26]
    out0_hbm, out1_hbm, out2 = refs[26:29]
    (
        owed, asked, all_sends, all_links, found, index,
        active0, hidden1, active1, out0, out1, halo0, halo1, grid1, grid2,
        own0, own1, own2, pooled0, pooled1,
        kernel0, weight0, weight1, weight2, hidden2, active2, halo2,
        choose_corners, choose_octants, place_matrix, shift_matrix,
        gathered, source, padded, moved,
    ) = refs[29:64]
    buffers = [refs[64 + 4 * n : 68 + 4 * n] for n in range(5)]
    masks, send_sems, recv_sems, local_sems, weight_sems = refs[84:]

    count = greet()
    fetch = pltpu.make_async_copy(kernel0_hbm, kernel0, local_sems.at[0])
    fetch.start()

    def blocks(level, kernel_hbm, weight):
        side = channels[level]
        return [
            pltpu.make_async_copy(
                kernel_hbm.at[n],
                weight.at[pl.ds(n // 9 * side, side), pl.ds(n % 9 * side, side)],
                weight_sems.at[level - 1, n],
            )
            for n in range(27)
        ]

    weights = blocks(1, kernel1_hbm, weight1) + blocks(2, kernel2_hbm, weight2)
    list_slots(sends, links, owed, asked)
    write_masks(masks, kinds)
    enter_fine(bricks[0], channels[0], voxels, gain0, faces, active0, own0)
    pl.semaphore_wait(pltpu.get_barrier_semaphore(), count)

    def meanwhile():
        resolve(found, all_links, all_sends, constants)
        depth = len(GROUPS) * 128
        at_row = lax.broadcasted_iota(I32, (depth, 128), 0)
        at_row = lax.shift_left(lax.shift_right_logical(at_row, 7), 6) + (at_row & 63)
        choose_corners[...] = jnp.where(at_row == corners[...], 1.0, 0.0).astype(BF16)
        tell = pltpu.make_async_copy(found, index, local_sems.at[2])
        tell.start()
        choose_octants[...] = selection(512, octants[...])
        shift_matrix[...] = selection(256, shifts[...])
        tell.wait()
        fetch.wait()
        arrange(channels[0], kernel0, weight0)
        for copy in weights:
            copy.start()

    def step(n, level, halo, base, own, out, **more):
        below = channels[level] if halo else channels[level - 1]
        size = bricks[level] * below
        wide = len(GROUPS) * 128 if halo else 512
        trade(
            bricks[level],
            below,
            own.shape[0],
            halo,
            base,
            own,
            index,
            out,
            *buffers[n],
            gathered.at[pl.ds(0, size // CHUNKS[n]), pl.ds(0, wide)],
            choose_corners if halo else choose_octants,
            masks,
            send_sems,
            recv_sems.at[n % 2],
            CHUNKS[n],
            **more,
        )

    def leave(level, active, halo, hidden, weight, out):
        size = bricks[level] * channels[level]
        convolve(
            bricks[level],
            channels[level],
            active,
            halo,
            hidden,
            weight,
            place_matrix,
            shift_matrix,
            out,
            source.at[pl.ds(0, size)],
            padded.at[pl.ds(0, size)],
            moved.at[pl.ds(0, 9 * channels[level])],
        )

    lines = [0, bricks[0], bricks[0] + bricks[1], sum(bricks), sum(bricks) + bricks[1]]
    step(
        0, 0, True, lines[0], own0, halo0, tables=(owed, asked, all_sends, all_links), meanwhile=meanwhile
    )
    place_matrix[...] = selection(1024, places[...])
    leave(0, active0, halo0, voxels, weight0, out0)
    keep0 = pltpu.make_async_copy(out0, out0_hbm, local_sems.at[3])
    keep0.start()
    pool(bricks[0], channels[0], out0, pooled0)
    step(1, 1, False, lines[3], pooled0, grid1)
    for copy in weights:
        copy.wait()
    enter_coarser(
        bricks[1], channels[0], channels[1], True, grid1, lift1, gain1, faces, hidden1, active1, own1
    )
    step(2, 1, True, lines[1], own1, halo1)
    leave(1, active1, halo1, hidden1, weight1, out1)
    keep1 = pltpu.make_async_copy(out1, out1_hbm, local_sems.at[4])
    keep1.start()
    pool(bricks[1], channels[1], out1, pooled1)
    step(3, 2, False, lines[4], pooled1, grid2)
    enter_coarser(
        bricks[2], channels[1], channels[2], False, grid2, lift2, gain2, faces, hidden2, active2, own2
    )
    step(4, 2, True, lines[2], own2, halo2)
    leave(2, active2, halo2, hidden2, weight2, out2)
    keep0.wait()
    keep1.wait()


def hand_on(*refs):
    for n in range(3):
        refs[3 + n][...] = refs[n][...]


def per_device(
    voxels_fine,
    gain_fine,
    gain_middle,
    gain_coarse,
    kernel_fine,
    kernel_middle,
    kernel_coarse,
    lift_middle,
    lift_coarse,
    links_fine,
    links_middle,
    links_coarse,
    sends_fine,
    sends_middle,
    sends_coarse,
    parents_middle,
    parents_coarse,
    uplinks_middle,
    uplinks_coarse,
):
    members = lax.axis_size("gx") * lax.axis_size("gy")
    bricks = [voxels_fine.shape[0], links_middle.shape[0], links_coarse.shape[0]]
    widths = [6 * bricks[0], 6 * bricks[1], 6 * bricks[2], bricks[0], bricks[1]]
    links = [links_fine, links_middle, links_coarse, parents_middle, parents_coarse]
    sends = [sends_fine, sends_middle, sends_coarse, uplinks_middle, uplinks_coarse]
    slots = [s.shape[1] // members for s in sends]
    rows = [t.shape[0] for t in links]
    constants = jnp.asarray(link_constants(tuple(zip(rows, widths, slots))))

    kernels = (kernel_fine, kernel_middle, kernel_coarse)
    channels = [k.shape[1] for k in kernels]
    sizes = [b * c for b, c in zip(bricks, channels)]
    places, shifts = jnp.asarray(padded_sources()), jnp.asarray(shift_sources())
    gains = [g.reshape(1, -1) for g in (gain_fine, gain_middle, gain_coarse)]
    hidden = voxels_fine.reshape(sizes[0], 512)

    def vmem(*dims, dtype=BF16):
        return pltpu.VMEM(dims, dtype)

    owns = [(3 * b, c, 128) for b, c in zip(bricks, channels)]
    pooled = [(bricks[n] // 2, channels[n], 128) for n in range(2)]
    grids = [bricks[n + 1] * channels[n] for n in range(2)]
    scratch = [
        vmem(2 * RING, SEND_ROWS, 128, dtype=I32),
        vmem(8, 128, dtype=I32),
        vmem(MEMBERS, SEND_ROWS, 128, dtype=I32),
        vmem(RING, 8, 128, dtype=I32),
        vmem(RING * LINK_ROWS, 128, dtype=I32),
        pltpu.SMEM((RING * LINK_ROWS, 128), I32),
        vmem(sizes[0], 512),
        vmem(sizes[1], 512),
        vmem(sizes[1], 512),
        vmem(sizes[0], 512),
        vmem(sizes[1], 512),
        vmem(sizes[0], 512),
        vmem(sizes[1], 512),
        vmem(grids[0], 512),
        vmem(grids[1], 512),
        vmem(*owns[0]),
        vmem(*owns[1]),
        vmem(*owns[2]),
        vmem(*pooled[0]),
        vmem(*pooled[1]),
        vmem(*kernel_fine.shape),
        vmem(3 * channels[0], 9 * channels[0]),
        vmem(3 * channels[1], 9 * channels[1]),
        vmem(3 * channels[2], 9 * channels[2]),
        vmem(sizes[2], 512),
        vmem(sizes[2], 512),
        vmem(sizes[2], 512),
        vmem(len(GROUPS) * 128, 128),
        vmem(512, 512),
        vmem(1024, 1280),
        vmem(256, 1152),
        vmem(max(sizes) // (1 if CHUNKS[0] == 1 else 2), len(GROUPS) * 128),
        vmem(max(sizes[:2]), 1024),
        vmem(max(sizes[:2]), 1280),
        vmem(9 * channels[2], 640),
    ]
    for table, size, chunks in zip(
        (owns[0], pooled[0], owns[1], pooled[1], owns[2]),
        (sizes[0], grids[0], sizes[1], grids[1], sizes[2]),
        CHUNKS,
    ):
        scratch += [
            vmem(MEMBERS * table[0] + 1, table[1], 128),
            vmem(RING, chunks, size // chunks, 512),
            vmem(chunks, size // chunks, 512),
            vmem(2, chunks, size // chunks, 512),
        ]
    scratch += [
        vmem(3 + 2 * len(KINDS), 16, 128),
        pltpu.SemaphoreType.DMA((COPIES,)),
        pltpu.SemaphoreType.DMA((2, COPIES)),
        pltpu.SemaphoreType.DMA((5,)),
        pltpu.SemaphoreType.DMA((2, 27)),
    ]
    anywhere = pl.BlockSpec(memory_space=pl.ANY)
    results = pl.pallas_call(
        functools.partial(body_kernel, bricks, channels),
        out_shape=[shape(size, 512) for size in sizes],
        in_specs=whole(23) + [anywhere] * 3,
        out_specs=[anywhere] * 2 + whole(1),
        scratch_shapes=scratch,
        compiler_params=pltpu.CompilerParams(
            collective_id=0, has_side_effects=True, vmem_limit_bytes=VMEM_LIMIT
        ),
        name="levels",
    )(
        hidden,
        *gains,
        lift_middle.T,
        lift_coarse,
        constants,
        jnp.asarray(face_sources()),
        jnp.asarray(corner_sources()),
        jnp.asarray(octant_sources()),
        places,
        shifts,
        jnp.asarray(kind_masks()),
        *sends,
        *links,
        *kernels,
    )
    outputs = pl.pallas_call(
        hand_on,
        out_shape=[shape(size, 512) for size in sizes],
        in_specs=whole(3),
        out_specs=whole(3),
        compiler_params=PARAMS,
        name="hand_on",
    )(*results)
    return tuple(
        out.reshape(b, c, 512) for out, b, c in zip(outputs, bricks, channels)
    )


def solution(mesh):
    split = ("gx", "gy")
    placed = (P(split, None, None),) + (P(),) * 8 + (P(split, None),) * 10
    return jax.shard_map(
        per_device,
        mesh=mesh,
        in_specs=placed,
        out_specs=(P(split, None, None),) * 3,
        check_vma=False,
    )
```
